32 devices in a mesh: ctx: 8 (over z, core), grp: 4 (over y, x).
Axes of the slice: x: 2, y: 2, z: 4, core: 2. Of those that a mesh axis runs over, the one named last changes fastest.
Arguments:
- queries: bfloat16 [2048, 8192], P('ctx', 'grp'), may hold values from -27 to 27, as said below
- keys: bfloat16 [2048, 1024], P('ctx'), may hold values from -27 to 27
- values: bfloat16 [2048, 1024], P('ctx'), may hold values from -6 to 6
- out_weight: bfloat16 [8192, 8192], P('grp'), may hold values from -0.0625 to 0.0625
- span_order: int32 [16], replicated, may hold values from 0 to 15, each once
- document: int32 [2048], replicated, may hold values from 0 to 3, never falling along the last dimension, each value on 1 to 1024 neighbouring positions
Outputs:
- projected: bfloat16 [2048, 8192], P('ctx', 'grp')
The draws below stay inside these ranges and needn't reach their ends.
Inputs may be any that keep to these rules, and one draw needn't show every extreme that they name: `queries`: queries and keys are of order one, except a few rows that may be larger.
All inputs are finite; a program needn't handle non-finite values.
Results may differ from the reference program's by a relative error of at most 0.023.
Values may be sent and summed in bfloat16 or wider, within the bound.
A program may use at most 128 MiB of HBM per device.

```python
import math
import jax
import jax.numpy as jnp
import numpy as np
from jax import lax

MODEL_DIM = 8192
Q_HEADS = 64
KV_HEADS = 8
HEAD_DIM = 128
QUERY_GROUP = 8
SPAN = 128
SEQ = 2048
N_CTX = 8
N_GRP = 4


def drawn_fields(key):
    base_query = jnp.clip(jax.random.normal(jax.random.fold_in(key, 11), (SEQ, Q_HEADS * HEAD_DIM), jnp.float32), -5.0, 5.0)
    base_key = jnp.clip(jax.random.normal(jax.random.fold_in(key, 12), (SEQ, KV_HEADS * HEAD_DIM), jnp.float32), -5.0, 5.0)
    return (base_query, base_key)


def draw_queries(key, part):
    return drawn_fields(key)[0].astype(jnp.bfloat16)


def draw_keys(key, part):
    return drawn_fields(key)[1].astype(jnp.bfloat16)


def block_scale(rng, dims, shards, low, top_value):
    factor_of, own = 1.0, jax.random.fold_in(rng, 6)
    for axis_at, blocks in shards:
        heights = jnp.exp(jax.random.uniform(jax.random.fold_in(own, axis_at), (blocks,), jnp.float32, low / len(shards), top_value / len(shards)))
        factor_of = factor_of * jnp.repeat(heights, dims[axis_at] // blocks).reshape([-1 if axis == axis_at else 1 for axis in range(len(dims))])
    return factor_of


def split_up(count, total, limit, skew):
    loads = [(1 << 20) // math.isqrt(rank ** skew) + 1 for rank in range(2, count + 1)]
    rest, counts = total - limit - (count - 1), [1] * (count - 1)
    while rest > 0:
        movable = [i for i in range(count - 1) if counts[i] < limit]
        mass, budget = sum([loads[i] for i in movable]), rest
        for i in movable:
            more = min(limit - counts[i], max(1, budget * loads[i] // mass), rest)
            counts[i] = counts[i] + more
            rest = rest - more
    return np.array([limit] + counts)


def ragged_sizes(own_key, number_of, total, reach, lean):
    if number_of == 2:
        one = jax.random.randint(own_key, (), max(1, total - reach), min(reach, total - 1) + 1)
        return jnp.stack([one, total - one])
    sizes = jnp.asarray(split_up(number_of, total, reach, lean), jnp.int32)
    twos = (number_of - 1) // 2
    donor, sink = sizes[1:1 + 2 * twos:2], sizes[2:2 + 2 * twos:2]
    slack = jnp.minimum(donor - 1, reach - sink)
    passed = jax.random.randint(jax.random.fold_in(own_key, 1), (twos,), 0, 1 << 20) % (slack + 1)
    sizes = sizes.at[1:1 + 2 * twos:2].set(donor - passed).at[2:2 + 2 * twos:2].set(sink + passed)
    return sizes[jax.random.permutation(jax.random.fold_in(own_key, 2), number_of)]


def bell_draw(own_key, dims, deviation, limit, cuts=(), kind=jnp.bfloat16):
    entries = deviation * jax.random.normal(own_key, dims, jnp.float32)
    if cuts:
        entries = entries * block_scale(own_key, dims, cuts, -0.22, 0.18)
    return jnp.clip(entries, -limit, limit).astype(kind)


def setup_inputs(seed: int = 0) -> dict:
    seeds = jax.random.split(jax.random.key(seed), 7)
    queries = draw_queries(jax.random.fold_in(seeds[6], 71), 0)
    keys = draw_keys(jax.random.fold_in(seeds[6], 71), 0)
    values = bell_draw(seeds[2], (SEQ, KV_HEADS * HEAD_DIM), 1.0, 6.0, ((0, 8),))
    out_weight = bell_draw(seeds[3], (Q_HEADS * HEAD_DIM, MODEL_DIM), (Q_HEADS * HEAD_DIM) ** -0.5, 0.0625, ((0, 4),))
    span_order = jax.random.permutation(seeds[4], 2 * N_CTX).astype(jnp.int32)
    document = jnp.searchsorted(jnp.cumsum(ragged_sizes(seeds[5], 4, SEQ, SEQ // 2, 0)), jnp.arange(SEQ), side="right").astype(jnp.int32)
    return dict(queries=queries, keys=keys, values=values, out_weight=out_weight, span_order=span_order, document=document)


def row_positions(span_order):
    rows = jnp.arange(SEQ, dtype=jnp.int32)
    return (span_order[rows // SPAN] * SPAN + rows % SPAN).astype(jnp.int32)

def reference(queries, keys, values, out_weight, span_order, document):
    positions = row_positions(span_order)
    docs = document[positions]
    visible = (positions[None, :] <= positions[:, None]) & (docs[None, :] == docs[:, None])
    score_scale = 1.0 / math.sqrt(HEAD_DIM)

    def one_head(head):
        shared = head // QUERY_GROUP
        query_head = lax.dynamic_slice_in_dim(queries, head * HEAD_DIM, HEAD_DIM, 1)
        key_head = lax.dynamic_slice_in_dim(keys, shared * HEAD_DIM, HEAD_DIM, 1)
        value_head = lax.dynamic_slice_in_dim(values, shared * HEAD_DIM, HEAD_DIM, 1)
        scores = jnp.dot(query_head, key_head.T, preferred_element_type=jnp.float32) * score_scale
        scores = jnp.where(visible, scores, -jnp.inf)
        highest = lax.optimization_barrier(jnp.max(scores, axis=1, keepdims=True))
        probs = jnp.exp(scores - highest)
        total = lax.optimization_barrier(jnp.sum(probs, axis=1, keepdims=True))
        mixed = jnp.dot(probs.astype(jnp.bfloat16), value_head, preferred_element_type=jnp.float32)
        return (mixed / total).astype(jnp.bfloat16)
    attended = lax.map(one_head, jnp.arange(Q_HEADS, dtype=jnp.int32))
    block_heads = Q_HEADS // N_GRP

    def add_block(running, block):
        head_rows = lax.dynamic_slice_in_dim(attended, block * block_heads, block_heads, 0)
        weight_rows = lax.dynamic_slice_in_dim(out_weight, block * block_heads * HEAD_DIM, block_heads * HEAD_DIM, 0)
        weight_rows = weight_rows.reshape(block_heads, HEAD_DIM, MODEL_DIM)
        block_sum = jnp.einsum('hsd,hdm->sm', head_rows.astype(jnp.float32), weight_rows.astype(jnp.float32))
        rounded = lax.optimization_barrier(block_sum.astype(jnp.bfloat16))
        return (running + rounded.astype(jnp.float32), None)
    start = jnp.zeros((SEQ, MODEL_DIM), jnp.float32)
    projected, unused = lax.scan(add_block, start, jnp.arange(N_GRP, dtype=jnp.int32))
    return projected.astype(jnp.bfloat16)
```

```python
import functools
import math
from types import SimpleNamespace

import jax
import jax.numpy as jnp
from jax import lax
from jax.experimental import pallas as pl
from jax.experimental.pallas import tpu as pltpu
from jax.sharding import PartitionSpec as P

HEAD_DIM = 128
QUERY_GROUP = 8
CORES = 2
MESH = pl.DeviceIdType.MESH
HIDDEN = -1e30
UNROLL = 4


def attention(
    n_ctx, kv_heads, first_of, greeted, order_ref, doc_rows, q_hbm, k_hbm, v_hbm,
    q_ref, kv_all, row_doc_ref, bias_ref, max_ref, acc_ref, local_sem, send_sem, recv_sem,
):
    nz = n_ctx // CORES
    me = lax.axis_index("ctx")
    group = lax.axis_index("grp")
    z, core = me // CORES, me % CORES
    partner = z * CORES + 1 - core
    tok_rows = kv_all.shape[2]
    span = doc_rows.shape[2]
    spans = tok_rows // span
    shared = q_ref.shape[1] // HEAD_DIM // kv_heads
    unroll = min(UNROLL, shared)
    factor = math.log2(math.e) / math.sqrt(HEAD_DIM)
    keys_per_step = CORES * tok_rows
    parts_of_keys = keys_per_step // HEAD_DIM
    near = jnp.minimum(z, nz - 1 - z)
    long_way = jnp.where(z < nz - 1 - z, 1, -1)

    def piece(way, h, chip, target):
        block = chip * CORES + core
        return pltpu.make_async_remote_copy(
            src_ref=kv_all.at[block, h],
            dst_ref=kv_all.at[block, h],
            send_sem=send_sem.at[way, h, chip],
            recv_sem=recv_sem.at[h, block],
            device_id=(target, group),
            device_id_type=MESH,
        )

    def arrived(h, chip, from_core):
        block = chip * CORES + from_core
        pltpu.make_async_copy(
            kv_all.at[block, h], kv_all.at[block, h], recv_sem.at[h, block]
        ).wait()

    def load(h, side):
        start = pl.multiple_of((first_of(group) + h) * HEAD_DIM, HEAD_DIM)
        return pltpu.make_async_copy(
            (k_hbm, v_hbm)[side].at[:, pl.ds(start, HEAD_DIM)],
            kv_all.at[me, h, :, pl.ds(side * HEAD_DIM, HEAD_DIM)],
            local_sem.at[h, side],
        )

    q_load = pltpu.make_async_copy(q_hbm, q_ref, local_sem.at[kv_heads, 0])

    def start():
        for h in range(kv_heads):
            for side in range(2):
                load(h, side).start()
        q_load.start()
        barrier = pltpu.get_barrier_semaphore()
        for target in [(partner, group)] + greeted:
            pl.semaphore_signal(barrier, inc=1, device_id=target, device_id_type=MESH)

        @pl.when(z > 0)
        def _():
            pl.semaphore_signal(
                barrier, inc=1, device_id=(me - CORES, group), device_id_type=MESH
            )

        @pl.when(z < nz - 1)
        def _():
            pl.semaphore_signal(
                barrier, inc=1, device_id=(me + CORES, group), device_id_type=MESH
            )

        pl.semaphore_wait(
            barrier, 1 + len(greeted) + jnp.minimum(z, 1) + jnp.minimum(nz - 1 - z, 1)
        )
        for h in range(kv_heads):
            for side in range(2):
                load(h, side).wait()

            @pl.when(z < nz - 1)
            def _():
                piece(0, h, z, me + CORES).start()

            @pl.when(z > 0)
            def _():
                piece(1, h, z, me - CORES).start()

            piece(2, h, z, partner).start()

    def prepare():
        max_ref[...] = jnp.full(max_ref.shape, HIDDEN, jnp.float32)
        acc_ref[...] = jnp.zeros(acc_ref.shape, jnp.float32)
        for r in range(spans):
            row_doc_ref[r] = jnp.transpose(
                jnp.broadcast_to(doc_rows[order_ref[me * spans + r]], (span, span))
            )
        q_load.wait()

    def pass_on(n, h):
        @pl.when((n > 0) & (z - n >= 0))
        def _():
            arrived(h, z - n, core)

            @pl.when(z < nz - 1)
            def _():
                piece(0, h, z - n, me + CORES).start()

            piece(2, h, z - n, partner).start()

        @pl.when((n > 0) & (z + n < nz))
        def _():
            arrived(h, z + n, core)

            @pl.when(z > 0)
            def _():
                piece(1, h, z + n, me - CORES).start()

            piece(2, h, z + n, partner).start()

    def chip_of(n):
        away = (n + 1) // 2
        paired = z + away * (1 - 2 * (n % 2))
        return jnp.where(n <= 2 * near, paired, z + long_way * (n - near))

    def look(chip):
        row_at = lax.broadcasted_iota(jnp.int32, (span, span), 0)
        col_at = lax.broadcasted_iota(jnp.int32, (span, span), 1)
        for slot in range(spans * CORES):
            key_span = order_ref[chip * (spans * CORES) + slot]
            key_doc = doc_rows[key_span]
            for r in range(spans):
                mine = order_ref[me * spans + r]
                seen = (key_doc == row_doc_ref[r]) & (
                    key_span * span + col_at <= mine * span + row_at
                )
                bias_ref[r * span : (r + 1) * span, slot * span : (slot + 1) * span] = jnp.where(
                    seen, 0.0, HIDDEN
                )

    def attend(chip, h, low, count):
        def some_heads(at, carry):
            both = kv_all[pl.ds(chip * CORES, CORES), h].reshape(keys_per_step, 2 * HEAD_DIM)
            key = both[:, :HEAD_DIM]
            value = both[:, HEAD_DIM:]
            value = jnp.concatenate([value, jnp.ones_like(value)], axis=1)
            picked = [h * shared + at * unroll + u for u in range(unroll)]
            rows = pl.ds(low, count)
            asked = jnp.concatenate(
                [
                    q_ref[rows, pl.ds(pl.multiple_of(head * HEAD_DIM, HEAD_DIM), HEAD_DIM)]
                    for head in picked
                ],
                axis=0,
            )
            scores = lax.dot_general(
                asked, key, (((1,), (1,)), ((), ())), preferred_element_type=jnp.float32
            )
            bias = bias_ref[rows, :]
            tops, rescales, probs = [], [], []
            for u, head in enumerate(picked):
                score = scores[u * count : (u + 1) * count] + bias
                old = max_ref[head, rows]
                top = jnp.maximum(old, jnp.max(score, axis=1, keepdims=True))
                tops.append(top)
                rescales.append(jnp.exp2((old - top) * factor))
                probs.append(
                    jnp.concatenate(
                        [
                            jnp.exp2(
                                (score[:, c * HEAD_DIM : (c + 1) * HEAD_DIM] - top) * factor
                            ).astype(jnp.bfloat16)
                            for c in range(parts_of_keys)
                        ],
                        axis=1,
                    )
                )
            mixed = jnp.dot(
                jnp.concatenate(probs, axis=0), value, preferred_element_type=jnp.float32
            )
            for u, head in enumerate(picked):
                max_ref[head, rows] = tops[u]
                scale = jnp.concatenate([rescales[u], rescales[u]], axis=1)
                acc_ref[head, rows] = (
                    acc_ref[head, rows] * scale + mixed[u * count : (u + 1) * count]
                )
            return carry

        lax.fori_loop(0, shared // unroll, some_heads, 0)

    def step(n, carry):
        chip = chip_of(n)
        look(chip)
        for h in range(kv_heads):
            pass_on(n, h)
            arrived(h, chip, 1 - core)
            attend(chip, h, 0, tok_rows)
        return carry

    def result(head, low, count):
        total = acc_ref[head, pl.ds(low, count)]
        return (total[:, :HEAD_DIM] / total[:, HEAD_DIM:]).astype(jnp.bfloat16)

    def drain():
        for h in range(kv_heads):
            for chip in range(nz):
                piece(2, h, chip, partner).wait_send()

                @pl.when((z < nz - 1) & (chip <= z))
                def _():
                    piece(0, h, chip, me + CORES).wait_send()

                @pl.when((z > 0) & (chip >= z))
                def _():
                    piece(1, h, chip, me - CORES).wait_send()

    return SimpleNamespace(**locals())


def attention_scratch(n_ctx, rows, heads, kv_heads, span):
    f32, bf16 = jnp.float32, jnp.bfloat16
    return [
        pltpu.VMEM((rows, heads * HEAD_DIM), bf16),
        pltpu.VMEM((n_ctx, kv_heads, rows, 2 * HEAD_DIM), bf16),
        pltpu.VMEM((rows // span, span, span), jnp.int32),
        pltpu.VMEM((rows, CORES * rows), f32),
        pltpu.VMEM((heads, rows, HEAD_DIM), f32),
        pltpu.VMEM((heads, rows, 2 * HEAD_DIM), f32),
        pltpu.SemaphoreType.DMA((kv_heads + 1, 2)),
        pltpu.SemaphoreType.DMA((3, kv_heads, n_ctx // CORES)),
        pltpu.SemaphoreType.DMA((kv_heads, n_ctx)),
    ]


def gather_attend_kernel(
    n_ctx, kv_heads, first_of, order_ref, doc_rows, q_hbm, k_hbm, v_hbm, out_ref, *scratch
):
    part = attention(
        n_ctx, kv_heads, first_of, [], order_ref, doc_rows, q_hbm, k_hbm, v_hbm, *scratch
    )
    part.start()
    part.prepare()
    lax.fori_loop(0, part.nz, part.step, 0)
    rows, width = out_ref.shape
    for head in range(width // HEAD_DIM):
        out_ref[:, head * HEAD_DIM : (head + 1) * HEAD_DIM] = part.result(head, 0, rows)
    part.drain()


def fused_kernel(
    n_ctx, kv_heads, first_of, order_ref, doc_rows, q_hbm, k_hbm, v_hbm, w_hbm, out_ref,
    att_ref, w_buf, send_one, got_one, send_two, got_two, own_ref,
    w_sem, sent_one, recv_one, sent_two, recv_two, *scratch,
):
    me = lax.axis_index("ctx")
    group = lax.axis_index("grp")
    side = group + 1 - 2 * (group % 2)
    other = (group + 2) % 4
    far = 3 - group
    pieces, _, width = w_buf.shape
    block_width = out_ref.shape[1]
    part = attention(
        n_ctx, kv_heads, first_of, [(me, side), (me, other)],
        order_ref, doc_rows, q_hbm, k_hbm, v_hbm, *scratch,
    )
    span, spans = part.span, part.spans
    heads = part.q_ref.shape[1] // HEAD_DIM

    def path_sub(i):
        path = i % 2
        return path, 2 * path + (i // 2) % 2

    def block_of(i):
        path = i % 2
        first = far if i < 4 else (other if path else side)
        return first if i < 8 else ((side if path else other) if i < 12 else group)

    def fetch(i, block, sub):
        start = pl.multiple_of(block * block_width + sub * width, width)
        return pltpu.make_async_copy(w_hbm.at[:, pl.ds(start, width)], w_buf.at[i], w_sem.at[i])

    def product(r, i):
        if r == 0:
            fetch(i, group, 0).wait()
        return jnp.dot(att_ref[r], w_buf[i], preferred_element_type=jnp.float32)

    def stage_one(r, i):
        path = i % 2
        return pltpu.make_async_remote_copy(
            src_ref=send_one.at[r, i],
            dst_ref=got_one.at[r, i],
            send_sem=sent_one.at[r, i],
            recv_sem=recv_one.at[r, i],
            device_id=(me, (1 - path) * side + path * other),
            device_id_type=MESH,
        )

    def stage_two(r, j):
        path = j % 2
        return pltpu.make_async_remote_copy(
            src_ref=send_two.at[r, j],
            dst_ref=got_two.at[r, j],
            send_sem=sent_two.at[r, j],
            recv_sem=recv_two.at[r, j],
            device_id=(me, (1 - path) * other + path * side),
            device_id_type=MESH,
        )

    def first(r, low, high):
        def one(i, carry):
            send_one[r, i] = product(r, i).astype(send_one.dtype)
            stage_one(r, i).start()
            return carry

        lax.fori_loop(low, high, one, 0)

    def second(r):
        def one(j, carry):
            value = product(r, 8 + j)
            stage_one(r, j).wait_recv()
            send_two[r, j] = (value + got_one[r, j].astype(jnp.float32)).astype(send_two.dtype)
            stage_two(r, j).start()
            return carry

        lax.fori_loop(0, 4, one, 0)

    def third(r):
        def one(j, carry):
            own_ref[r, j] = product(r, 12 + j)
            return carry

        lax.fori_loop(0, 4, one, 0)

    def add_first(r):
        for j in range(4):
            stage_one(r, 4 + j).wait_recv()
            own_ref[r, j] = own_ref[r, j] + got_one[r, 4 + j].astype(jnp.float32)

    def last(r):
        for j in range(4):
            stage_two(r, j).wait_recv()
            at = path_sub(j)[1] * width
            out_ref[r * span : (r + 1) * span, at : at + width] = (
                own_ref[r, j] + got_two[r, j].astype(jnp.float32)
            ).astype(out_ref.dtype)

    def normalise(r):
        for head in range(heads):
            att_ref[r, :, head * HEAD_DIM : (head + 1) * HEAD_DIM] = part.result(
                head, r * span, span
            )

    part.start()
    for i in range(pieces):
        fetch(i, block_of(i), path_sub(i)[1]).start()
    part.prepare()
    lax.fori_loop(0, part.nz - 1, part.step, 0)

    n = part.nz - 1
    chip = part.chip_of(n)
    part.look(chip)
    for h in range(kv_heads - 1):
        part.pass_on(n, h)
        part.arrived(h, chip, 1 - part.core)
        part.attend(chip, h, 0, spans * span)
    part.pass_on(n, kv_heads - 1)
    part.arrived(kv_heads - 1, chip, 1 - part.core)
    part.attend(chip, kv_heads - 1, 0, span)
    normalise(0)
    first(0, 0, 8)
    part.attend(chip, kv_heads - 1, span, span)
    normalise(1)
    first(1, 0, 4)
    second(0)
    first(1, 4, 8)
    third(0)
    second(1)
    third(1)
    add_first(0)
    last(0)
    add_first(1)
    last(1)
    for r in range(spans):
        for i in range(8):
            stage_one(r, i).wait_send()
        for j in range(4):
            stage_two(r, j).wait_send()
    part.drain()


def fused(queries, keys, values, out_weight, span_order, document, n_ctx, kv_heads, first_of):
    slots = span_order.shape[0]
    span = document.shape[0] // slots
    rows, depth = queries.shape
    features = out_weight.shape[1]
    width = features // 16
    spans = rows // span
    f32, bf16 = jnp.float32, jnp.bfloat16
    hbm = pl.BlockSpec(memory_space=pl.ANY)
    vmem = pl.BlockSpec(memory_space=pltpu.VMEM)
    return pl.pallas_call(
        functools.partial(fused_kernel, n_ctx, kv_heads, first_of),
        out_shape=jax.ShapeDtypeStruct((rows, features // 4), bf16),
        in_specs=[pl.BlockSpec(memory_space=pltpu.SMEM), vmem, hbm, hbm, hbm, hbm],
        out_specs=vmem,
        scratch_shapes=[
            pltpu.VMEM((spans, span, depth), bf16),
            pltpu.VMEM((16, depth, width), bf16),
            pltpu.VMEM((spans, 8, span, width), bf16),
            pltpu.VMEM((spans, 8, span, width), bf16),
            pltpu.VMEM((spans, 4, span, width), bf16),
            pltpu.VMEM((spans, 4, span, width), bf16),
            pltpu.VMEM((spans, 4, span, width), f32),
            pltpu.SemaphoreType.DMA((16,)),
            pltpu.SemaphoreType.DMA((spans, 8)),
            pltpu.SemaphoreType.DMA((spans, 8)),
            pltpu.SemaphoreType.DMA((spans, 4)),
            pltpu.SemaphoreType.DMA((spans, 4)),
        ]
        + attention_scratch(n_ctx, rows, depth // HEAD_DIM, kv_heads, span),
        compiler_params=pltpu.CompilerParams(
            collective_id=0, has_side_effects=True, vmem_limit_bytes=60 * 1024 * 1024
        ),
        name="attend_project",
    )(span_order, document.reshape(slots, 1, span), queries, keys, values, out_weight)


def gather_attend(queries, keys, values, span_order, document, n_ctx, kv_heads, first_of):
    slots = span_order.shape[0]
    span = document.shape[0] // slots
    rows, depth = queries.shape
    hbm = pl.BlockSpec(memory_space=pl.ANY)
    vmem = pl.BlockSpec(memory_space=pltpu.VMEM)
    return pl.pallas_call(
        functools.partial(gather_attend_kernel, n_ctx, kv_heads, first_of),
        out_shape=jax.ShapeDtypeStruct(queries.shape, queries.dtype),
        in_specs=[pl.BlockSpec(memory_space=pltpu.SMEM), vmem, hbm, hbm, hbm],
        out_specs=vmem,
        scratch_shapes=attention_scratch(n_ctx, rows, depth // HEAD_DIM, kv_heads, span),
        compiler_params=pltpu.CompilerParams(collective_id=0, has_side_effects=True),
        name="gather_attend",
    )(span_order, document.reshape(slots, 1, span), queries, keys, values)


def shards(n_ctx, n_grp, queries, keys, values, out_weight, span_order, document):
    local_heads = queries.shape[1] // HEAD_DIM
    kv_heads = max(1, local_heads // QUERY_GROUP)

    def first_of(group):
        return group * local_heads // QUERY_GROUP

    if n_grp == 4:
        return fused(
            queries, keys, values, out_weight, span_order, document, n_ctx, kv_heads, first_of
        )
    attended = gather_attend(
        queries, keys, values, span_order, document, n_ctx, kv_heads, first_of
    )
    partial_value = jnp.dot(attended, out_weight, preferred_element_type=jnp.float32)
    return lax.psum_scatter(
        partial_value.astype(jnp.bfloat16), "grp", scatter_dimension=1, tiled=True
    )


def solution(mesh):
    in_specs = (P("ctx", "grp"), P("ctx", None), P("ctx", None), P("grp", None), P(), P())
    body = functools.partial(shards, mesh.shape["ctx"], mesh.shape["grp"])
    return jax.shard_map(
        body, mesh=mesh, in_specs=in_specs, out_specs=P("ctx", "grp"), check_vma=False
    )
```

```python
import functools
import math
from types import SimpleNamespace

import jax
import jax.numpy as jnp
from jax import lax
from jax.experimental import pallas as pl
from jax.experimental.pallas import tpu as pltpu
from jax.sharding import PartitionSpec as P

HEAD_DIM = 128
QUERY_GROUP = 8
CORES = 2
MESH = pl.DeviceIdType.MESH
HIDDEN = -1e30
UNROLL = 4


def attention(
    n_ctx, kv_heads, first_of, greeted, order_ref, doc_rows, q_hbm, k_hbm, v_hbm,
    q_ref, kv_all, row_doc_ref, bias_ref, max_ref, acc_ref, local_sem, send_sem, recv_sem,
):
    nz = n_ctx // CORES
    me = lax.axis_index("ctx")
    group = lax.axis_index("grp")
    z, core = me // CORES, me % CORES
    partner = z * CORES + 1 - core
    tok_rows = kv_all.shape[2]
    span = doc_rows.shape[2]
    spans = tok_rows // span
    shared = q_ref.shape[1] // HEAD_DIM // kv_heads
    unroll = min(UNROLL, shared)
    groups = shared // unroll
    factor = math.log2(math.e) / math.sqrt(HEAD_DIM)
    keys_per_step = CORES * tok_rows
    parts_of_keys = keys_per_step // HEAD_DIM
    near = jnp.minimum(z, nz - 1 - z)
    long_way = jnp.where(z < nz - 1 - z, 1, -1)

    def piece(way, h, chip, target):
        block = chip * CORES + core
        return pltpu.make_async_remote_copy(
            src_ref=kv_all.at[block, h],
            dst_ref=kv_all.at[block, h],
            send_sem=send_sem.at[way, h, chip],
            recv_sem=recv_sem.at[h, block],
            device_id=(target, group),
            device_id_type=MESH,
        )

    def arrived(h, chip, from_core):
        block = chip * CORES + from_core
        pltpu.make_async_copy(
            kv_all.at[block, h], kv_all.at[block, h], recv_sem.at[h, block]
        ).wait()

    def load(h, side):
        start = pl.multiple_of((first_of(group) + h) * HEAD_DIM, HEAD_DIM)
        return pltpu.make_async_copy(
            (k_hbm, v_hbm)[side].at[:, pl.ds(start, HEAD_DIM)],
            kv_all.at[me, h, :, pl.ds(side * HEAD_DIM, HEAD_DIM)],
            local_sem.at[h, side],
        )

    q_load = pltpu.make_async_copy(q_hbm, q_ref, local_sem.at[kv_heads, 0])

    def start():
        for h in range(kv_heads):
            for side in range(2):
                load(h, side).start()
        q_load.start()
        barrier = pltpu.get_barrier_semaphore()
        for target in [(partner, group)] + greeted:
            pl.semaphore_signal(barrier, inc=1, device_id=target, device_id_type=MESH)

        @pl.when(z > 0)
        def _():
            pl.semaphore_signal(
                barrier, inc=1, device_id=(me - CORES, group), device_id_type=MESH
            )

        @pl.when(z < nz - 1)
        def _():
            pl.semaphore_signal(
                barrier, inc=1, device_id=(me + CORES, group), device_id_type=MESH
            )

        pl.semaphore_wait(
            barrier, 1 + len(greeted) + jnp.minimum(z, 1) + jnp.minimum(nz - 1 - z, 1)
        )
        for h in range(kv_heads):
            for side in range(2):
                load(h, side).wait()

            @pl.when(z < nz - 1)
            def _():
                piece(0, h, z, me + CORES).start()

            @pl.when(z > 0)
            def _():
                piece(1, h, z, me - CORES).start()

            piece(2, h, z, partner).start()

    def prepare():
        max_ref[...] = jnp.full(max_ref.shape, HIDDEN, jnp.float32)
        acc_ref[...] = jnp.zeros(acc_ref.shape, jnp.float32)
        for r in range(spans):
            row_doc_ref[r] = jnp.transpose(
                jnp.broadcast_to(doc_rows[order_ref[me * spans + r]], (span, span))
            )
        q_load.wait()

    def pass_on(n, h):
        @pl.when((n > 0) & (z - n >= 0))
        def _():
            arrived(h, z - n, core)

            @pl.when(z < nz - 1)
            def _():
                piece(0, h, z - n, me + CORES).start()

            piece(2, h, z - n, partner).start()

        @pl.when((n > 0) & (z + n < nz))
        def _():
            arrived(h, z + n, core)

            @pl.when(z > 0)
            def _():
                piece(1, h, z + n, me - CORES).start()

            piece(2, h, z + n, partner).start()

    def chip_of(n):
        away = (n + 1) // 2
        paired = z + away * (1 - 2 * (n % 2))
        return jnp.where(n <= 2 * near, paired, z + long_way * (n - near))

    def look(chip):
        row_at = lax.broadcasted_iota(jnp.int32, (span, span), 0)
        col_at = lax.broadcasted_iota(jnp.int32, (span, span), 1)
        for slot in range(spans * CORES):
            key_span = order_ref[chip * (spans * CORES) + slot]
            key_doc = doc_rows[key_span]
            for r in range(spans):
                mine = order_ref[me * spans + r]
                seen = (key_doc == row_doc_ref[r]) & (
                    key_span * span + col_at <= mine * span + row_at
                )
                bias_ref[r * span : (r + 1) * span, slot * span : (slot + 1) * span] = jnp.where(
                    seen, 0.0, HIDDEN
                )

    def attend(chip, h, at, low, count):
        rows = pl.ds(low, count)
        both = kv_all[pl.ds(chip * CORES, CORES), h].reshape(keys_per_step, 2 * HEAD_DIM)
        key = both[:, :HEAD_DIM]
        value = both[:, HEAD_DIM:]
        value = jnp.concatenate([value, jnp.ones_like(value)], axis=1)
        picked = [h * shared + at * unroll + u for u in range(unroll)]
        scores = [
            lax.dot_general(
                q_ref[rows, pl.ds(pl.multiple_of(head * HEAD_DIM, HEAD_DIM), HEAD_DIM)],
                key,
                (((1,), (1,)), ((), ())),
                preferred_element_type=jnp.float32,
            )
            + bias_ref[rows, :]
            for head in picked
        ]
        olds = [max_ref[head, rows] for head in picked]
        sums = [acc_ref[head, rows] for head in picked]
        results = []
        for score, old, total in zip(scores, olds, sums):
            top = jnp.maximum(old, jnp.max(score, axis=1, keepdims=True))
            rescale = jnp.exp2((old - top) * factor)
            probs = jnp.concatenate(
                [
                    jnp.exp2(
                        (score[:, c * HEAD_DIM : (c + 1) * HEAD_DIM] - top) * factor
                    ).astype(jnp.bfloat16)
                    for c in range(parts_of_keys)
                ],
                axis=1,
            )
            mixed = jnp.dot(probs, value, preferred_element_type=jnp.float32)
            scale = jnp.concatenate([rescale, rescale], axis=1)
            results.append((top, total * scale + mixed))
        for head, (top, total) in zip(picked, results):
            max_ref[head, rows] = top
            acc_ref[head, rows] = total

    def attend_many(chip, h, first, stop, low, count):
        def one(at, carry):
            attend(chip, h, at, low, count)
            return carry

        lax.fori_loop(first, stop, one, 0)

    def take(k, early):
        n, h = k // kv_heads, k % kv_heads
        before = k - 1
        with jax.named_scope("pass_on"):
            pass_on(n, h)
        with jax.named_scope("rest"):
            attend_many(chip_of(before // kv_heads), before % kv_heads, early, groups, 0, tok_rows)

        @pl.when(h == 0)
        def _():
            look(chip_of(n))

        with jax.named_scope("arrive"):
            arrived(h, chip_of(n), 1 - core)

    def steps(early, stop):
        look(z)
        arrived(0, z, 1 - core)
        attend_many(z, 0, 0, early, 0, tok_rows)

        def one(k, carry):
            take(k, early)
            with jax.named_scope("attend"):
                attend_many(chip_of(k // kv_heads), k % kv_heads, 0, early, 0, tok_rows)
            return carry

        lax.fori_loop(1, stop, one, 0)

    def result(head, low, count):
        total = acc_ref[head, pl.ds(low, count)]
        return (total[:, :HEAD_DIM] / total[:, HEAD_DIM:]).astype(jnp.bfloat16)

    def drain():
        for h in range(kv_heads):
            for chip in range(nz):
                piece(2, h, chip, partner).wait_send()

                @pl.when((z < nz - 1) & (chip <= z))
                def _():
                    piece(0, h, chip, me + CORES).wait_send()

                @pl.when((z > 0) & (chip >= z))
                def _():
                    piece(1, h, chip, me - CORES).wait_send()

    return SimpleNamespace(**locals())


def attention_scratch(n_ctx, rows, heads, kv_heads, span):
    f32, bf16 = jnp.float32, jnp.bfloat16
    return [
        pltpu.VMEM((rows, heads * HEAD_DIM), bf16),
        pltpu.VMEM((n_ctx, kv_heads, rows, 2 * HEAD_DIM), bf16),
        pltpu.VMEM((rows // span, span, span), jnp.int32),
        pltpu.VMEM((rows, CORES * rows), f32),
        pltpu.VMEM((heads, rows, HEAD_DIM), f32),
        pltpu.VMEM((heads, rows, 2 * HEAD_DIM), f32),
        pltpu.SemaphoreType.DMA((kv_heads + 1, 2)),
        pltpu.SemaphoreType.DMA((3, kv_heads, n_ctx // CORES)),
        pltpu.SemaphoreType.DMA((kv_heads, n_ctx)),
    ]


def gather_attend_kernel(
    n_ctx, kv_heads, first_of, order_ref, doc_rows, q_hbm, k_hbm, v_hbm, out_ref, *scratch
):
    part = attention(
        n_ctx, kv_heads, first_of, [], order_ref, doc_rows, q_hbm, k_hbm, v_hbm, *scratch
    )
    part.start()
    part.prepare()
    part.steps(part.groups, part.nz * kv_heads)
    rows, width = out_ref.shape
    for head in range(width // HEAD_DIM):
        out_ref[:, head * HEAD_DIM : (head + 1) * HEAD_DIM] = part.result(head, 0, rows)
    part.drain()


def fused_kernel(
    n_ctx, kv_heads, first_of, order_ref, doc_rows, q_hbm, k_hbm, v_hbm, w_hbm, out_ref,
    att_ref, w_buf, send_one, got_one, send_two, got_two, own_ref,
    w_sem, sent_one, recv_one, sent_two, recv_two, *scratch,
):
    me = lax.axis_index("ctx")
    group = lax.axis_index("grp")
    side = group + 1 - 2 * (group % 2)
    other = (group + 2) % 4
    far = 3 - group
    pieces, _, width = w_buf.shape
    block_width = out_ref.shape[1]
    part = attention(
        n_ctx, kv_heads, first_of, [(me, side), (me, other)],
        order_ref, doc_rows, q_hbm, k_hbm, v_hbm, *scratch,
    )
    span, spans = part.span, part.spans
    heads = part.q_ref.shape[1] // HEAD_DIM

    def path_sub(i):
        path = i % 2
        return path, 2 * path + (i // 2) % 2

    def block_of(i):
        path = i % 2
        first = far if i < 4 else (other if path else side)
        return first if i < 8 else ((side if path else other) if i < 12 else group)

    def fetch(i, block, sub):
        start = pl.multiple_of(block * block_width + sub * width, width)
        return pltpu.make_async_copy(w_hbm.at[:, pl.ds(start, width)], w_buf.at[i], w_sem.at[i])

    def product(r, i):
        if r == 0:
            fetch(i, group, 0).wait()
        return jnp.dot(att_ref[r], w_buf[i], preferred_element_type=jnp.float32)

    def stage_one(r, i):
        path = i % 2
        return pltpu.make_async_remote_copy(
            src_ref=send_one.at[r, i],
            dst_ref=got_one.at[r, i],
            send_sem=sent_one.at[r, i],
            recv_sem=recv_one.at[r, i],
            device_id=(me, (1 - path) * side + path * other),
            device_id_type=MESH,
        )

    def stage_two(r, j):
        path = j % 2
        return pltpu.make_async_remote_copy(
            src_ref=send_two.at[r, j],
            dst_ref=got_two.at[r, j],
            send_sem=sent_two.at[r, j],
            recv_sem=recv_two.at[r, j],
            device_id=(me, (1 - path) * other + path * side),
            device_id_type=MESH,
        )

    def first(r, low, high):
        def one(i, carry):
            send_one[r, i] = product(r, i).astype(send_one.dtype)
            stage_one(r, i).start()
            return carry

        lax.fori_loop(low, high, one, 0)

    def second(r):
        def one(j, carry):
            value = product(r, 8 + j)
            stage_one(r, j).wait_recv()
            send_two[r, j] = (value + got_one[r, j].astype(jnp.float32)).astype(send_two.dtype)
            stage_two(r, j).start()
            return carry

        lax.fori_loop(0, 4, one, 0)

    def third(r):
        def one(j, carry):
            own_ref[r, j] = product(r, 12 + j)
            return carry

        lax.fori_loop(0, 4, one, 0)

    def add_first(r):
        for j in range(4):
            stage_one(r, 4 + j).wait_recv()
            own_ref[r, j] = own_ref[r, j] + got_one[r, 4 + j].astype(jnp.float32)

    def last(r):
        for j in range(4):
            stage_two(r, j).wait_recv()
            at = path_sub(j)[1] * width
            out_ref[r * span : (r + 1) * span, at : at + width] = (
                own_ref[r, j] + got_two[r, j].astype(jnp.float32)
            ).astype(out_ref.dtype)

    def normalise(r):
        for head in range(heads):
            att_ref[r, :, head * HEAD_DIM : (head + 1) * HEAD_DIM] = part.result(
                head, r * span, span
            )

    with jax.named_scope("begin"):
        part.start()
    for i in range(pieces):
        fetch(i, block_of(i), path_sub(i)[1]).start()
    with jax.named_scope("prepare"):
        part.prepare()
    final = part.nz * kv_heads - 1
    early = (part.groups + 1) // 2
    part.steps(early, final)
    part.take(final, early)
    chip = part.chip_of(part.nz - 1)
    with jax.named_scope("attend_last"):
        part.attend_many(chip, kv_heads - 1, 0, part.groups, 0, span)
        normalise(0)
    with jax.named_scope("first_0"):
        first(0, 0, 8)
    with jax.named_scope("attend_1"):
        part.attend_many(chip, kv_heads - 1, 0, part.groups, span, span)
        normalise(1)
    with jax.named_scope("first_1_far"):
        first(1, 0, 4)
    with jax.named_scope("second_0"):
        second(0)
    with jax.named_scope("first_1_near"):
        first(1, 4, 8)
    with jax.named_scope("third_0"):
        third(0)
    with jax.named_scope("second_1"):
        second(1)
    with jax.named_scope("third_1"):
        third(1)
    with jax.named_scope("add_0"):
        add_first(0)
    with jax.named_scope("last_0"):
        last(0)
    with jax.named_scope("add_1"):
        add_first(1)
    with jax.named_scope("last_1"):
        last(1)
    with jax.named_scope("drain"):
        for r in range(spans):
            for i in range(8):
                stage_one(r, i).wait_send()
            for j in range(4):
                stage_two(r, j).wait_send()
        part.drain()


def fused(queries, keys, values, out_weight, span_order, document, n_ctx, kv_heads, first_of):
    slots = span_order.shape[0]
    span = document.shape[0] // slots
    rows, depth = queries.shape
    features = out_weight.shape[1]
    width = features // 16
    spans = rows // span
    f32, bf16 = jnp.float32, jnp.bfloat16
    hbm = pl.BlockSpec(memory_space=pl.ANY)
    vmem = pl.BlockSpec(memory_space=pltpu.VMEM)
    return pl.pallas_call(
        functools.partial(fused_kernel, n_ctx, kv_heads, first_of),
        out_shape=pltpu.VMEM((rows, features // 4), bf16),
        in_specs=[pl.BlockSpec(memory_space=pltpu.SMEM), vmem, hbm, hbm, hbm, hbm],
        out_specs=vmem,
        scratch_shapes=[
            pltpu.VMEM((spans, span, depth), bf16),
            pltpu.VMEM((16, depth, width), bf16),
            pltpu.VMEM((spans, 8, span, width), bf16),
            pltpu.VMEM((spans, 8, span, width), bf16),
            pltpu.VMEM((spans, 4, span, width), bf16),
            pltpu.VMEM((spans, 4, span, width), bf16),
            pltpu.VMEM((spans, 4, span, width), f32),
            pltpu.SemaphoreType.DMA((16,)),
            pltpu.SemaphoreType.DMA((spans, 8)),
            pltpu.SemaphoreType.DMA((spans, 8)),
            pltpu.SemaphoreType.DMA((spans, 4)),
            pltpu.SemaphoreType.DMA((spans, 4)),
        ]
        + attention_scratch(n_ctx, rows, depth // HEAD_DIM, kv_heads, span),
        compiler_params=pltpu.CompilerParams(
            collective_id=0, has_side_effects=True, vmem_limit_bytes=60 * 1024 * 1024
        ),
        name="attend_project",
    )(span_order, document.reshape(slots, 1, span), queries, keys, values, out_weight)


def gather_attend(queries, keys, values, span_order, document, n_ctx, kv_heads, first_of):
    slots = span_order.shape[0]
    span = document.shape[0] // slots
    rows, depth = queries.shape
    hbm = pl.BlockSpec(memory_space=pl.ANY)
    vmem = pl.BlockSpec(memory_space=pltpu.VMEM)
    return pl.pallas_call(
        functools.partial(gather_attend_kernel, n_ctx, kv_heads, first_of),
        out_shape=jax.ShapeDtypeStruct(queries.shape, queries.dtype),
        in_specs=[pl.BlockSpec(memory_space=pltpu.SMEM), vmem, hbm, hbm, hbm],
        out_specs=vmem,
        scratch_shapes=attention_scratch(n_ctx, rows, depth // HEAD_DIM, kv_heads, span),
        compiler_params=pltpu.CompilerParams(collective_id=0, has_side_effects=True),
        name="gather_attend",
    )(span_order, document.reshape(slots, 1, span), queries, keys, values)


def shards(n_ctx, n_grp, queries, keys, values, out_weight, span_order, document):
    local_heads = queries.shape[1] // HEAD_DIM
    kv_heads = max(1, local_heads // QUERY_GROUP)

    def first_of(group):
        return group * local_heads // QUERY_GROUP

    if n_grp == 4:
        return fused(
            queries, keys, values, out_weight, span_order, document, n_ctx, kv_heads, first_of
        )
    attended = gather_attend(
        queries, keys, values, span_order, document, n_ctx, kv_heads, first_of
    )
    partial_value = jnp.dot(attended, out_weight, preferred_element_type=jnp.float32)
    return lax.psum_scatter(
        partial_value.astype(jnp.bfloat16), "grp", scatter_dimension=1, tiled=True
    )


def solution(mesh):
    in_specs = (P("ctx", "grp"), P("ctx", None), P("ctx", None), P("grp", None), P(), P())
    body = functools.partial(shards, mesh.shape["ctx"], mesh.shape["grp"])
    return jax.shard_map(
        body, mesh=mesh, in_specs=in_specs, out_specs=P("ctx", "grp"), check_vma=False
    )
```

```python
import functools
import math
from types import SimpleNamespace

import jax
import jax.numpy as jnp
from jax import lax
from jax.experimental import pallas as pl
from jax.experimental.pallas import tpu as pltpu
from jax.sharding import PartitionSpec as P

HEAD_DIM = 128
QUERY_GROUP = 8
CORES = 2
MESH = pl.DeviceIdType.MESH
HIDDEN = -1e30
UNROLL = 4


def attention(
    n_ctx, kv_heads, first_of, greeted, order_hbm, doc_hbm, q_hbm, k_hbm, v_hbm,
    order_ref, doc_rows, q_ref, kv_all, row_doc_ref, bias_ref, max_ref, acc_ref,
    local_sem, send_sem, recv_sem,
):
    nz = n_ctx // CORES
    me = lax.axis_index("ctx")
    group = lax.axis_index("grp")
    z, core = me // CORES, me % CORES
    partner = z * CORES + 1 - core
    tok_rows = kv_all.shape[2]
    span = doc_rows.shape[2]
    spans = tok_rows // span
    shared = q_ref.shape[1] // HEAD_DIM // kv_heads
    unroll = min(UNROLL, shared)
    groups = shared // unroll
    factor = math.log2(math.e) / math.sqrt(HEAD_DIM)
    keys_per_step = CORES * tok_rows
    parts_of_keys = keys_per_step // HEAD_DIM
    near = jnp.minimum(z, nz - 1 - z)
    long_way = jnp.where(z < nz - 1 - z, 1, -1)

    def piece(way, h, chip, target):
        block = chip * CORES + core
        return pltpu.make_async_remote_copy(
            src_ref=kv_all.at[block, h],
            dst_ref=kv_all.at[block, h],
            send_sem=send_sem.at[way // 2],
            recv_sem=recv_sem.at[h, block],
            device_id=(target, group),
            device_id_type=MESH,
        )

    def arrived(h, chip, from_core):
        block = chip * CORES + from_core
        pltpu.make_async_copy(
            kv_all.at[block, h], kv_all.at[block, h], recv_sem.at[h, block]
        ).wait()

    def load(h, side):
        start = pl.multiple_of((first_of(group) + h) * HEAD_DIM, HEAD_DIM)
        return pltpu.make_async_copy(
            (k_hbm, v_hbm)[side].at[:, pl.ds(start, HEAD_DIM)],
            kv_all.at[me, h, :, pl.ds(side * HEAD_DIM, HEAD_DIM)],
            local_sem.at[h],
        )

    def loaded(h):
        pltpu.make_async_copy(kv_all.at[me, h], kv_all.at[me, h], local_sem.at[h]).wait()

    q_load = pltpu.make_async_copy(q_hbm, q_ref, local_sem.at[kv_heads])
    order_load = pltpu.make_async_copy(order_hbm, order_ref, local_sem.at[kv_heads + 1])
    doc_load = pltpu.make_async_copy(doc_hbm, doc_rows, local_sem.at[kv_heads + 2])

    def start():
        for h in range(kv_heads):
            for side in range(2):
                load(h, side).start()
        order_load.start()
        doc_load.start()
        q_load.start()
        barrier = pltpu.get_barrier_semaphore()
        for target in [(partner, group)] + greeted:
            pl.semaphore_signal(barrier, inc=1, device_id=target, device_id_type=MESH)

        @pl.when(z > 0)
        def _():
            pl.semaphore_signal(
                barrier, inc=1, device_id=(me - CORES, group), device_id_type=MESH
            )

        @pl.when(z < nz - 1)
        def _():
            pl.semaphore_signal(
                barrier, inc=1, device_id=(me + CORES, group), device_id_type=MESH
            )

        pl.semaphore_wait(
            barrier, 1 + len(greeted) + jnp.minimum(z, 1) + jnp.minimum(nz - 1 - z, 1)
        )
        for h in range(kv_heads):
            loaded(h)

            @pl.when(z < nz - 1)
            def _():
                piece(0, h, z, me + CORES).start()

            @pl.when(z > 0)
            def _():
                piece(1, h, z, me - CORES).start()

            piece(2, h, z, partner).start()

    def prepare():
        max_ref[...] = jnp.full(max_ref.shape, HIDDEN, jnp.float32)
        acc_ref[...] = jnp.zeros(acc_ref.shape, jnp.float32)
        order_load.wait()
        doc_load.wait()
        for r in range(spans):
            row_doc_ref[r] = jnp.transpose(
                jnp.broadcast_to(doc_rows[order_ref[me * spans + r]], (span, span))
            )
        q_load.wait()

    def pass_on(n, h):
        @pl.when((n > 0) & (z - n >= 0))
        def _():
            arrived(h, z - n, core)

            @pl.when(z < nz - 1)
            def _():
                piece(0, h, z - n, me + CORES).start()

            piece(2, h, z - n, partner).start()

        @pl.when((n > 0) & (z + n < nz))
        def _():
            arrived(h, z + n, core)

            @pl.when(z > 0)
            def _():
                piece(1, h, z + n, me - CORES).start()

            piece(2, h, z + n, partner).start()

    def chip_of(n):
        away = (n + 1) // 2
        paired = z + away * (1 - 2 * (n % 2))
        return jnp.where(n <= 2 * near, paired, z + long_way * (n - near))

    def look(chip):
        row_at = lax.broadcasted_iota(jnp.int32, (span, span), 0)
        col_at = lax.broadcasted_iota(jnp.int32, (span, span), 1)
        for slot in range(spans * CORES):
            key_span = order_ref[chip * (spans * CORES) + slot]
            key_doc = doc_rows[key_span]
            for r in range(spans):
                mine = order_ref[me * spans + r]
                seen = (key_doc == row_doc_ref[r]) & (
                    key_span * span + col_at <= mine * span + row_at
                )
                bias_ref[r * span : (r + 1) * span, slot * span : (slot + 1) * span] = jnp.where(
                    seen, 0.0, HIDDEN
                )

    def attend(chip, h, at, low, count):
        rows = pl.ds(low, count)
        both = kv_all[pl.ds(chip * CORES, CORES), h].reshape(keys_per_step, 2 * HEAD_DIM)
        key = both[:, :HEAD_DIM]
        value = both[:, HEAD_DIM:]
        value = jnp.concatenate([value, jnp.ones_like(value)], axis=1)
        picked = [h * shared + at * unroll + u for u in range(unroll)]
        scores = [
            lax.dot_general(
                q_ref[rows, pl.ds(pl.multiple_of(head * HEAD_DIM, HEAD_DIM), HEAD_DIM)],
                key,
                (((1,), (1,)), ((), ())),
                preferred_element_type=jnp.float32,
            )
            + bias_ref[rows, :]
            for head in picked
        ]
        olds = [max_ref[head, rows] for head in picked]
        sums = [acc_ref[head, rows] for head in picked]
        results = []
        for score, old, total in zip(scores, olds, sums):
            top = jnp.maximum(old, jnp.max(score, axis=1, keepdims=True))
            rescale = jnp.exp2((old - top) * factor)
            probs = jnp.concatenate(
                [
                    jnp.exp2(
                        (score[:, c * HEAD_DIM : (c + 1) * HEAD_DIM] - top) * factor
                    ).astype(jnp.bfloat16)
                    for c in range(parts_of_keys)
                ],
                axis=1,
            )
            mixed = jnp.dot(probs, value, preferred_element_type=jnp.float32)
            scale = jnp.concatenate([rescale, rescale], axis=1)
            results.append((top, total * scale + mixed))
        for head, (top, total) in zip(picked, results):
            max_ref[head, rows] = top
            acc_ref[head, rows] = total

    def attend_many(chip, h, first, stop, low, count):
        def one(at, carry):
            attend(chip, h, at, low, count)
            return carry

        lax.fori_loop(first, stop, one, 0)

    def take(k, early):
        n, h = k // kv_heads, k % kv_heads
        before = k - 1
        with jax.named_scope("pass_on"):
            pass_on(n, h)
        with jax.named_scope("rest"):
            attend_many(chip_of(before // kv_heads), before % kv_heads, early, groups, 0, tok_rows)

        @pl.when(h == 0)
        def _():
            look(chip_of(n))

        with jax.named_scope("arrive"):
            arrived(h, chip_of(n), 1 - core)

    def steps(early, stop):
        look(z)
        arrived(0, z, 1 - core)
        attend_many(z, 0, 0, early, 0, tok_rows)

        def one(k, carry):
            take(k, early)
            with jax.named_scope("attend"):
                attend_many(chip_of(k // kv_heads), k % kv_heads, 0, early, 0, tok_rows)
            return carry

        lax.fori_loop(1, stop, one, 0)

    def result(head, low, count):
        total = acc_ref[head, pl.ds(low, count)]
        return (total[:, :HEAD_DIM] / total[:, HEAD_DIM:]).astype(jnp.bfloat16)

    def drain():
        pltpu.make_async_copy(kv_all.at[:nz], kv_all.at[:nz], send_sem.at[1]).wait()
        for at in range(nz):
            sent = (at + 1) * (at < nz - 1) + (nz - at) * (at > 0)

            @pl.when(z == at)
            def _():
                blocks = kv_all.at[:sent]
                pltpu.make_async_copy(blocks, blocks, send_sem.at[0]).wait()

    return SimpleNamespace(**locals())


def attention_scratch(n_ctx, slots, rows, heads, kv_heads, span):
    f32, bf16 = jnp.float32, jnp.bfloat16
    return [
        pltpu.SMEM((slots,), jnp.int32),
        pltpu.VMEM((slots, 1, span), jnp.int32),
        pltpu.VMEM((rows, heads * HEAD_DIM), bf16),
        pltpu.VMEM((n_ctx, kv_heads, rows, 2 * HEAD_DIM), bf16),
        pltpu.VMEM((rows // span, span, span), jnp.int32),
        pltpu.VMEM((rows, CORES * rows), f32),
        pltpu.VMEM((heads, rows, HEAD_DIM), f32),
        pltpu.VMEM((heads, rows, 2 * HEAD_DIM), f32),
        pltpu.SemaphoreType.DMA((kv_heads + 3,)),
        pltpu.SemaphoreType.DMA((2,)),
        pltpu.SemaphoreType.DMA((kv_heads, n_ctx)),
    ]


def gather_attend_kernel(
    n_ctx, kv_heads, first_of, order_hbm, doc_hbm, q_hbm, k_hbm, v_hbm, out_ref, *scratch
):
    part = attention(
        n_ctx, kv_heads, first_of, [], order_hbm, doc_hbm, q_hbm, k_hbm, v_hbm, *scratch
    )
    part.start()
    part.prepare()
    part.steps(part.groups, part.nz * kv_heads)
    rows, width = out_ref.shape
    for head in range(width // HEAD_DIM):
        out_ref[:, head * HEAD_DIM : (head + 1) * HEAD_DIM] = part.result(head, 0, rows)
    part.drain()


def fused_kernel(
    n_ctx, kv_heads, first_of, order_hbm, doc_hbm, q_hbm, k_hbm, v_hbm, w_hbm, out_ref,
    att_ref, w_buf, send_ref, got_ref, own_ref,
    w_sem, sent_sem, far_sem, near_sem, two_sem, *scratch,
):
    me = lax.axis_index("ctx")
    group = lax.axis_index("grp")
    side = group + 1 - 2 * (group % 2)
    other = (group + 2) % 4
    far = 3 - group
    pieces, _, width = w_buf.shape
    block_width = out_ref.shape[1]
    part = attention(
        n_ctx, kv_heads, first_of, [(me, side), (me, other)],
        order_hbm, doc_hbm, q_hbm, k_hbm, v_hbm, *scratch,
    )
    spans, span = att_ref.shape[:2]
    heads = part.q_ref.shape[1] // HEAD_DIM

    def path_sub(i):
        path = i % 2
        return path, 2 * path + (i // 2) % 2

    def block_of(i):
        path = i % 2
        first = far if i < 4 else (other if path else side)
        return first if i < 8 else ((side if path else other) if i < 12 else group)

    def fetch(i, block, sub):
        start = pl.multiple_of(block * block_width + sub * width, width)
        return pltpu.make_async_copy(
            w_hbm.at[:, pl.ds(start, width)], w_buf.at[i], w_sem.at[i // 8]
        )

    def fetched(half):
        part_of = w_buf.at[pl.ds(half * 8, 8)]
        pltpu.make_async_copy(part_of, part_of, w_sem.at[half]).wait()

    def product(r, i):
        return jnp.dot(att_ref[r], w_buf[i], preferred_element_type=jnp.float32)

    def send(r, i, path, sem):
        return pltpu.make_async_remote_copy(
            src_ref=send_ref.at[r, i],
            dst_ref=got_ref.at[r, i],
            send_sem=sent_sem.at[0],
            recv_sem=sem,
            device_id=(me, (1 - path) * side + path * other),
            device_id_type=MESH,
        )

    def got(r, low, count, sem):
        part_of = got_ref.at[r, pl.ds(low, count)]
        pltpu.make_async_copy(part_of, part_of, sem).wait()

    def first_far(r):
        def one(i, carry):
            send_ref[r, i] = product(r, i).astype(send_ref.dtype)
            send(r, i, i % 2, far_sem.at[r, i]).start()
            return carry

        lax.fori_loop(0, 4, one, 0)

    def first_near(r):
        def one(i, carry):
            send_ref[r, i] = product(r, i).astype(send_ref.dtype)
            send(r, i, i % 2, near_sem.at[r]).start()
            return carry

        lax.fori_loop(4, 8, one, 0)

    def second(r):
        def one(i, carry):
            value = product(r, i)
            got(r, i - 8, 1, far_sem.at[r, i - 8])
            send_ref[r, i] = (value + got_ref[r, i - 8].astype(jnp.float32)).astype(
                send_ref.dtype
            )
            send(r, i, 1 - i % 2, two_sem.at[r, i - 8]).start()
            return carry

        lax.fori_loop(8, 12, one, 0)

    def third(r):
        def one(j, carry):
            own_ref[r, j] = product(r, 12 + j)
            return carry

        lax.fori_loop(0, 4, one, 0)

    def add_first(r):
        got(r, 4, 4, near_sem.at[r])
        for j in range(4):
            own_ref[r, j] = own_ref[r, j] + got_ref[r, 4 + j].astype(jnp.float32)

    def last(r):
        for j in range(4):
            got(r, 8 + j, 1, two_sem.at[r, j])
            at = path_sub(j)[1] * width
            out_ref[r * span : (r + 1) * span, at : at + width] = (
                own_ref[r, j] + got_ref[r, 8 + j].astype(jnp.float32)
            ).astype(out_ref.dtype)

    def normalise(r, first, stop):
        for head in range(first, stop):
            att_ref[r, :, head * HEAD_DIM : (head + 1) * HEAD_DIM] = part.result(
                head, r * span, span
            )

    with jax.named_scope("begin"):
        part.start()
    for i in range(pieces):
        fetch(i, block_of(i), path_sub(i)[1]).start()
    with jax.named_scope("prepare"):
        part.prepare()
    final = part.nz * kv_heads - 1
    early = (part.groups + 1) // 2
    done = (kv_heads - 1) * part.shared
    part.steps(early, final)
    part.take(final, early)
    chip = part.chip_of(part.nz - 1)
    with jax.named_scope("attend_last"):
        part.attend_many(chip, kv_heads - 1, 0, part.groups, 0, span)
    with jax.named_scope("norm"):
        normalise(0, 0, heads)
    with jax.named_scope("first_0"):
        fetched(0)
        first_far(0)
        first_near(0)
    with jax.named_scope("attend_1"):
        part.attend_many(chip, kv_heads - 1, 0, part.groups, span, span)
        normalise(1, 0, heads)
    with jax.named_scope("first_1_far"):
        first_far(1)
        fetched(1)
    with jax.named_scope("second_0"):
        second(0)
    with jax.named_scope("first_1_near"):
        first_near(1)
    with jax.named_scope("third_0"):
        third(0)
    with jax.named_scope("second_1"):
        second(1)
    with jax.named_scope("third_1"):
        third(1)
    with jax.named_scope("add_0"):
        add_first(0)
    with jax.named_scope("last_0"):
        last(0)
    with jax.named_scope("add_1"):
        add_first(1)
    with jax.named_scope("last_1"):
        last(1)
    with jax.named_scope("drain"):
        pltpu.make_async_copy(send_ref, send_ref, sent_sem.at[0]).wait()
        part.drain()


def fused(queries, keys, values, out_weight, span_order, document, n_ctx, kv_heads, first_of):
    slots = span_order.shape[0]
    span = document.shape[0] // slots
    rows, depth = queries.shape
    features = out_weight.shape[1]
    width = features // 16
    spans = rows // span
    f32, bf16 = jnp.float32, jnp.bfloat16
    hbm = pl.BlockSpec(memory_space=pl.ANY)
    vmem = pl.BlockSpec(memory_space=pltpu.VMEM)
    return pl.pallas_call(
        functools.partial(fused_kernel, n_ctx, kv_heads, first_of),
        out_shape=pltpu.VMEM((rows, features // 4), bf16),
        in_specs=[hbm] * 6,
        out_specs=vmem,
        scratch_shapes=[
            pltpu.VMEM((spans, span, depth), bf16),
            pltpu.VMEM((16, depth, width), bf16),
            pltpu.VMEM((spans, 12, span, width), bf16),
            pltpu.VMEM((spans, 12, span, width), bf16),
            pltpu.VMEM((spans, 4, span, width), f32),
            pltpu.SemaphoreType.DMA((2,)),
            pltpu.SemaphoreType.DMA((1,)),
            pltpu.SemaphoreType.DMA((spans, 4)),
            pltpu.SemaphoreType.DMA((spans,)),
            pltpu.SemaphoreType.DMA((spans, 4)),
        ]
        + attention_scratch(n_ctx, slots, rows, depth // HEAD_DIM, kv_heads, span),
        compiler_params=pltpu.CompilerParams(
            collective_id=0, has_side_effects=True, vmem_limit_bytes=60 * 1024 * 1024
        ),
        name="attend_project",
    )(span_order, document.reshape(slots, 1, span), queries, keys, values, out_weight)


def gather_attend(queries, keys, values, span_order, document, n_ctx, kv_heads, first_of):
    slots = span_order.shape[0]
    span = document.shape[0] // slots
    rows, depth = queries.shape
    hbm = pl.BlockSpec(memory_space=pl.ANY)
    vmem = pl.BlockSpec(memory_space=pltpu.VMEM)
    return pl.pallas_call(
        functools.partial(gather_attend_kernel, n_ctx, kv_heads, first_of),
        out_shape=jax.ShapeDtypeStruct(queries.shape, queries.dtype),
        in_specs=[hbm] * 5,
        out_specs=vmem,
        scratch_shapes=attention_scratch(n_ctx, slots, rows, depth // HEAD_DIM, kv_heads, span),
        compiler_params=pltpu.CompilerParams(collective_id=0, has_side_effects=True),
        name="gather_attend",
    )(span_order, document.reshape(slots, 1, span), queries, keys, values)


def shards(n_ctx, n_grp, queries, keys, values, out_weight, span_order, document):
    local_heads = queries.shape[1] // HEAD_DIM
    kv_heads = max(1, local_heads // QUERY_GROUP)

    def first_of(group):
        return group * local_heads // QUERY_GROUP

    if n_grp == 4:
        return fused(
            queries, keys, values, out_weight, span_order, document, n_ctx, kv_heads, first_of
        )
    attended = gather_attend(
        queries, keys, values, span_order, document, n_ctx, kv_heads, first_of
    )
    partial_value = jnp.dot(attended, out_weight, preferred_element_type=jnp.float32)
    return lax.psum_scatter(
        partial_value.astype(jnp.bfloat16), "grp", scatter_dimension=1, tiled=True
    )


def solution(mesh):
    in_specs = (P("ctx", "grp"), P("ctx", None), P("ctx", None), P("grp", None), P(), P())
    body = functools.partial(shards, mesh.shape["ctx"], mesh.shape["grp"])
    return jax.shard_map(
        body, mesh=mesh, in_specs=in_specs, out_specs=P("ctx", "grp"), check_vma=False
    )
```

```python
import functools
import math
from types import SimpleNamespace

import jax
import jax.numpy as jnp
from jax import lax
from jax.experimental import pallas as pl
from jax.experimental.pallas import tpu as pltpu
from jax.sharding import PartitionSpec as P

HEAD_DIM = 128
QUERY_GROUP = 8
CORES = 2
MESH = pl.DeviceIdType.MESH
HIDDEN = -1e30
ONES = 16


def attention(
    n_ctx, kv_heads, first_of, greeted, order_hbm, doc_hbm, q_hbm, k_hbm, v_hbm,
    order_ref, doc_rows, q_ref, kv_all, turned_ref, doc_cols, bias_ref, max_ref, acc_ref,
    local_sem, send_sem, recv_sem,
    few_q=None, more_q=None, more_doc=None, more_bias=None, more_max=None, more_acc=None,
    more_sem=None,
):
    nz = n_ctx // CORES
    me = lax.axis_index("ctx")
    group = lax.axis_index("grp")
    z, core = me // CORES, me % CORES
    partner = z * CORES + 1 - core
    tok_rows = kv_all.shape[2]
    span = doc_rows.shape[2]
    spans = tok_rows // span
    shared = q_ref.shape[1] // HEAD_DIM // kv_heads
    factor = math.log2(math.e) / math.sqrt(HEAD_DIM)
    keys_per_step = CORES * tok_rows
    near = jnp.minimum(z, nz - 1 - z)
    extra = HEAD_DIM // shared
    kept = span - extra
    mate = (z + 1 - 2 * (z % 2)) * CORES + core
    long_way = jnp.where(z < nz - 1 - z, 1, -1)

    def piece(way, h, chip, target):
        block = chip * CORES + core
        return pltpu.make_async_remote_copy(
            src_ref=kv_all.at[block, h],
            dst_ref=kv_all.at[block, h],
            send_sem=send_sem.at[way // 2],
            recv_sem=recv_sem.at[h, block],
            device_id=(target, group),
            device_id_type=MESH,
        )

    def arrived(h, chip, from_core):
        block = chip * CORES + from_core
        pltpu.make_async_copy(
            kv_all.at[block, h], kv_all.at[block, h], recv_sem.at[h, block]
        ).wait()

    def load(h, side):
        start = pl.multiple_of((first_of(group) + h) * HEAD_DIM, HEAD_DIM)
        return pltpu.make_async_copy(
            (k_hbm, v_hbm)[side].at[:, pl.ds(start, HEAD_DIM)],
            kv_all.at[me, h, :, pl.ds(side * HEAD_DIM, HEAD_DIM)],
            local_sem.at[h],
        )

    def loaded(h):
        pltpu.make_async_copy(kv_all.at[me, h], kv_all.at[me, h], local_sem.at[h]).wait()

    q_load = pltpu.make_async_copy(q_hbm, q_ref, local_sem.at[kv_heads])
    order_load = pltpu.make_async_copy(order_hbm, order_ref, local_sem.at[kv_heads + 1])
    doc_load = pltpu.make_async_copy(doc_hbm, doc_rows, local_sem.at[kv_heads + 2])

    def lend():
        return pltpu.make_async_remote_copy(
            src_ref=more_q,
            dst_ref=more_q,
            send_sem=more_sem.at[0],
            recv_sem=more_sem.at[1],
            device_id=(mate, group),
            device_id_type=MESH,
        )

    few_load = (
        None if more_q is None else
        pltpu.make_async_copy(q_hbm.at[pl.ds(kept, extra)], few_q, more_sem.at[2])
    )

    def stage():
        for head in range(kv_heads * shared):
            h, u = head // shared, head % shared
            more_q[h, u * extra : (u + 1) * extra] = few_q[
                :, head * HEAD_DIM : (head + 1) * HEAD_DIM
            ]
        lend().start()

    def start():
        for h in range(kv_heads):
            for side in range(2):
                load(h, side).start()
        order_load.start()
        doc_load.start()
        if few_load is not None:
            few_load.start()
        q_load.start()
        barrier = pltpu.get_barrier_semaphore()
        for target in [(partner, group)] + greeted:
            pl.semaphore_signal(barrier, inc=1, device_id=target, device_id_type=MESH)

        @pl.when(z > 0)
        def _():
            pl.semaphore_signal(
                barrier, inc=1, device_id=(me - CORES, group), device_id_type=MESH
            )

        @pl.when(z < nz - 1)
        def _():
            pl.semaphore_signal(
                barrier, inc=1, device_id=(me + CORES, group), device_id_type=MESH
            )

        pl.semaphore_wait(
            barrier, 1 + len(greeted) + jnp.minimum(z, 1) + jnp.minimum(nz - 1 - z, 1)
        )
        for h in range(kv_heads):
            loaded(h)

            @pl.when(z < nz - 1)
            def _():
                piece(0, h, z, me + CORES).start()

            @pl.when(z > 0)
            def _():
                piece(1, h, z, me - CORES).start()

            piece(2, h, z, partner).start()
            if h == 0 and few_load is not None:
                few_load.wait()
                pl.when(near == 0)(stage)

    def prepare():
        max_ref[...] = jnp.full(max_ref.shape, HIDDEN, jnp.float32)
        acc_ref[...] = jnp.zeros(acc_ref.shape, jnp.float32)
        order_load.wait()
        doc_load.wait()
        turned_ref[:, HEAD_DIM:] = jnp.ones((kv_heads, ONES, keys_per_step), turned_ref.dtype)
        for at in range(doc_rows.shape[0]):
            doc_cols[at] = jnp.transpose(jnp.broadcast_to(doc_rows[at], (span, span)))
        if more_q is not None:
            more_max[...] = jnp.full(more_max.shape, HIDDEN, jnp.float32)
            more_acc[...] = jnp.zeros(more_acc.shape, jnp.float32)
            theirs = jnp.broadcast_to(doc_rows[lent_span()], more_doc.shape)
            lane = lax.broadcasted_iota(jnp.int32, more_doc.shape, 1)
            rolled = theirs
            for u in range(shared):
                moved = pltpu.roll(theirs, (u * extra - kept) % span, 1)
                rolled = jnp.where(lane // extra == u, moved, rolled)
            more_doc[...] = rolled
        q_load.wait()

    def pass_on(n, h):
        def from_below():
            arrived(h, z - n, core)

            @pl.when(z < nz - 1)
            def _():
                piece(0, h, z - n, me + CORES).start()

            piece(2, h, z - n, partner).start()

        def from_above():
            arrived(h, z + n, core)

            @pl.when(z > 0)
            def _():
                piece(1, h, z + n, me - CORES).start()

            piece(2, h, z + n, partner).start()

        above_first = z < nz - 1 - z
        pl.when((n > 0) & (z + n < nz) & above_first)(from_above)
        pl.when((n > 0) & (z - n >= 0))(from_below)
        pl.when((n > 0) & (z + n < nz) & jnp.logical_not(above_first))(from_above)

    def chip_of(n):
        away = (n + 1) // 2
        paired = z + away * (1 - 2 * (n % 2))
        return jnp.where(n <= 2 * near, paired, z + long_way * (n - near))

    def lent_span():
        return order_ref[jnp.where(near == 1, mate, me) * spans]

    def look(chip):
        key_at = lax.broadcasted_iota(jnp.int32, (span, span), 0)
        row_at = lax.broadcasted_iota(jnp.int32, (span, span), 1)
        for slot in range(spans * CORES):
            key_span = order_ref[chip * (spans * CORES) + slot]
            key_doc = doc_cols[key_span]
            for r in range(spans):
                mine = order_ref[me * spans + r]
                seen = (key_doc == doc_rows[mine]) & (
                    key_span * span + key_at <= mine * span + row_at
                )
                bias_ref[slot * span : (slot + 1) * span, r * span : (r + 1) * span] = jnp.where(
                    seen, 0.0, HIDDEN
                )
            if more_q is not None:
                seen = (key_doc == more_doc[:1]) & (
                    key_span * span + key_at <= lent_span() * span + kept + row_at % extra
                )
                more_bias[slot * span : (slot + 1) * span] = jnp.where(seen, 0.0, HIDDEN)

    def turn(block, blocks, h):
        both = kv_all[pl.ds(block, blocks), h].reshape(blocks * tok_rows, 2 * HEAD_DIM)
        turned_ref[h, :HEAD_DIM] = jnp.transpose(both[:, HEAD_DIM:])

    def attend(chip, h, low, count, own=True, lent=False):
        rows = pl.ds(low, count)
        key = kv_all[pl.ds(chip * CORES, CORES), h].reshape(keys_per_step, 2 * HEAD_DIM)
        key = key[:, :HEAD_DIM]
        asked = []
        if own:
            for u in range(shared):
                head = h * shared + u
                at = pl.ds(pl.multiple_of(head * HEAD_DIM, HEAD_DIM), HEAD_DIM)
                asked.append(
                    (q_ref[rows, at], bias_ref, max_ref.at[head], acc_ref.at[head], rows)
                )
        if lent:
            every = slice(None)
            asked.append((more_q[h], more_bias, more_max.at[h], more_acc.at[h], every))
        scores = [
            lax.dot_general(
                key, query, (((1,), (1,)), ((), ())), preferred_element_type=jnp.float32
            )
            + bias[:, at]
            for query, bias, _, _, at in asked
        ]
        for (_, _, maxes, sums, at), score in zip(asked, scores):
            old = maxes[:, at]
            top = jnp.maximum(old, jnp.max(score, axis=0, keepdims=True))
            rescale = jnp.exp2((old - top) * factor)
            probs = jnp.exp2((score - top) * factor).astype(jnp.bfloat16)
            mixed = jnp.dot(turned_ref[h], probs, preferred_element_type=jnp.float32)
            maxes[:, at] = top
            sums[:, at] = sums[:, at] * rescale + mixed

    def plan(k):
        middle = near == 1
        after = k - 2
        first_n = jnp.where(
            middle, 2 * (after >= 2), (after > 0) * (k + 1) // 2
        )
        first_h = jnp.where(middle, after == 3, (after > 0) * (k + 1) % 2)
        second_n = jnp.where(after == 0, 1, 0)
        chip = jnp.where(
            middle & (after >= 0), chip_of(1 + after % 2), chip_of(k // kv_heads)
        )
        held = jnp.where(middle & (after >= 0), after // 2, k % kv_heads)
        return first_n, first_h.astype(jnp.int32), second_n, chip, held

    def slots(begin, stop, lent):
        def one(k, carry):
            first_n, first_h, second_n, chip, held = plan(k)
            with jax.named_scope("pass_on"):
                pass_on(first_n, first_h)
                pass_on(second_n, 1)
            look(chip)
            with jax.named_scope("arrive"):
                arrived(held, chip, 1 - core)
            turn(chip * CORES, CORES, held)
            with jax.named_scope("attend"):
                attend(chip, held, 0, tok_rows, lent=lent)
            return carry

        lax.fori_loop(begin, stop, one, 0)

    def steps():
        def one(k, carry):
            n, h = k // kv_heads, k % kv_heads
            pass_on(n, h)
            look(chip_of(n))
            arrived(h, chip_of(n), 1 - core)
            turn(chip_of(n) * CORES, CORES, h)
            attend(chip_of(n), h, 0, tok_rows)
            return carry

        lax.fori_loop(0, nz * kv_heads, one, 0)

    def finished(total):
        scale = 1.0 / total[HEAD_DIM : HEAD_DIM + 1]
        return jnp.transpose((total[:HEAD_DIM] * scale).astype(jnp.bfloat16))

    def result(head, low, count):
        return finished(acc_ref[head, :, pl.ds(low, count)])

    def drain():
        pltpu.make_async_copy(kv_all.at[:nz], kv_all.at[:nz], send_sem.at[1]).wait()
        for at in range(nz):
            sent = (at + 1) * (at < nz - 1) + (nz - at) * (at > 0)

            @pl.when(z == at)
            def _():
                blocks = kv_all.at[:sent]
                pltpu.make_async_copy(blocks, blocks, send_sem.at[0]).wait()

    return SimpleNamespace(**locals())


def attention_scratch(n_ctx, slots, rows, heads, kv_heads, span):
    f32, bf16 = jnp.float32, jnp.bfloat16
    return [
        pltpu.SMEM((slots,), jnp.int32),
        pltpu.VMEM((slots, 1, span), jnp.int32),
        pltpu.VMEM((rows, heads * HEAD_DIM), bf16),
        pltpu.VMEM((n_ctx, kv_heads, rows, 2 * HEAD_DIM), bf16),
        pltpu.VMEM((kv_heads, HEAD_DIM + ONES, CORES * rows), bf16),
        pltpu.VMEM((slots, span, span), jnp.int32),
        pltpu.VMEM((CORES * rows, rows), f32),
        pltpu.VMEM((heads, 1, rows), f32),
        pltpu.VMEM((heads, HEAD_DIM + ONES, rows), f32),
        pltpu.SemaphoreType.DMA((kv_heads + 3,)),
        pltpu.SemaphoreType.DMA((2,)),
        pltpu.SemaphoreType.DMA((kv_heads, n_ctx)),
    ]


def gather_attend_kernel(
    n_ctx, kv_heads, first_of, order_hbm, doc_hbm, q_hbm, k_hbm, v_hbm, out_ref, *scratch
):
    part = attention(
        n_ctx, kv_heads, first_of, [], order_hbm, doc_hbm, q_hbm, k_hbm, v_hbm, *scratch
    )
    part.start()
    part.prepare()
    part.steps()
    rows, width = out_ref.shape
    for head in range(width // HEAD_DIM):
        out_ref[:, head * HEAD_DIM : (head + 1) * HEAD_DIM] = part.result(head, 0, rows)
    part.drain()


def fused_kernel(
    n_ctx, kv_heads, first_of, order_hbm, doc_hbm, q_hbm, k_hbm, v_hbm, w_hbm, out_ref,
    att_ref, w_buf, send_ref, got_ref, own_ref, back_out, back_in,
    w_sem, sent_sem, far_sem, near_sem, two_sem, back_sem, *scratch,
):
    me = lax.axis_index("ctx")
    group = lax.axis_index("grp")
    side = group + 1 - 2 * (group % 2)
    other = (group + 2) % 4
    far = 3 - group
    pieces, _, width = w_buf.shape
    block_width = out_ref.shape[1]
    part = attention(
        n_ctx, kv_heads, first_of, [(me, side), (me, other)],
        order_hbm, doc_hbm, q_hbm, k_hbm, v_hbm, *scratch,
    )
    span, spans, extra, kept, shared = part.span, part.spans, part.extra, part.kept, part.shared
    middle = part.near == 1

    def path_sub(i):
        path = i % 2
        return path, 2 * path + (i // 2) % 2

    def block_of(i):
        path = i % 2
        first = far if i < 4 else (other if path else side)
        return first if i < 8 else ((side if path else other) if i < 12 else group)

    def fetch(i, block, sub):
        start = pl.multiple_of(block * block_width + sub * width, width)
        return pltpu.make_async_copy(
            w_hbm.at[:, pl.ds(start, width)], w_buf.at[i], w_sem.at[i // 8]
        )

    def fetched(half):
        part_of = w_buf.at[pl.ds(half * 8, 8)]
        pltpu.make_async_copy(part_of, part_of, w_sem.at[half]).wait()

    def held_rows(r):
        return span if r else span + extra

    def sized(r, do):
        if r:
            do(span)
        else:
            pl.when(middle)(lambda: do(span + extra))
            pl.when(jnp.logical_not(middle))(lambda: do(kept))

    def product(r, i):
        return jnp.dot(
            att_ref[r, : held_rows(r)], w_buf[i], preferred_element_type=jnp.float32
        )

    def send(r, i, path, sem):
        sized(
            r,
            lambda count: pltpu.make_async_remote_copy(
                src_ref=send_ref.at[r, i, :count],
                dst_ref=got_ref.at[r, i, :count],
                send_sem=sent_sem.at[r],
                recv_sem=sem,
                device_id=(me, (1 - path) * side + path * other),
                device_id_type=MESH,
            ).start(),
        )

    def got(r, low, pieces_of, sem):
        def wait(count):
            part_of = got_ref.at[r, pl.ds(low, pieces_of), :count]
            pltpu.make_async_copy(part_of, part_of, sem).wait()

        sized(r, wait)

    def sent(r):
        def wait(count):
            part_of = send_ref.at[r, :, :count]
            pltpu.make_async_copy(part_of, part_of, sent_sem.at[r]).wait()

        sized(r, wait)

    def give_back():
        return pltpu.make_async_remote_copy(
            src_ref=back_out,
            dst_ref=back_in,
            send_sem=back_sem.at[0],
            recv_sem=back_sem.at[1],
            device_id=(part.mate, group),
            device_id_type=MESH,
        )

    def first_far(r):
        def one(i, carry):
            send_ref[r, i, : held_rows(r)] = product(r, i).astype(send_ref.dtype)
            send(r, i, i % 2, far_sem.at[r, i])
            return carry

        lax.fori_loop(0, 4, one, 0)

    def first_near(r):
        def one(i, carry):
            send_ref[r, i, : held_rows(r)] = product(r, i).astype(send_ref.dtype)
            send(r, i, i % 2, near_sem.at[r])
            return carry

        lax.fori_loop(4, 8, one, 0)

    def second(r):
        def one(i, carry):
            value = product(r, i)
            got(r, i - 8, 1, far_sem.at[r, i - 8])
            count = held_rows(r)
            send_ref[r, i, :count] = (
                value + got_ref[r, i - 8, :count].astype(jnp.float32)
            ).astype(send_ref.dtype)
            send(r, i, 1 - i % 2, two_sem.at[r, i - 8])
            return carry

        lax.fori_loop(8, 12, one, 0)

    def third(r):
        def one(j, carry):
            own_ref[r, j, : held_rows(r)] = product(r, 12 + j)
            return carry

        lax.fori_loop(0, 4, one, 0)

    def add_first(r):
        got(r, 4, 4, near_sem.at[r])
        for j in range(4):
            count = held_rows(r)
            own_ref[r, j, :count] = own_ref[r, j, :count] + got_ref[r, 4 + j, :count].astype(
                jnp.float32
            )

    def last(r):
        for j in range(4):
            got(r, 8 + j, 1, two_sem.at[r, j])
            at = path_sub(j)[1] * width
            total = (
                own_ref[r, j, : held_rows(r)]
                + got_ref[r, 8 + j, : held_rows(r)].astype(jnp.float32)
            ).astype(out_ref.dtype)
            if r:
                out_ref[span:, at : at + width] = total
            else:
                out_ref[:kept, at : at + width] = total[:kept]

                @pl.when(middle)
                def _():
                    out_ref[kept:span, at : at + width] = total[kept:span]
                    back_out[:, at : at + width] = total[span:]

    def normalise(r, h):
        for head in range(h * shared, (h + 1) * shared):
            att_ref[r, :span, head * HEAD_DIM : (head + 1) * HEAD_DIM] = part.result(
                head, r * span, span
            )
        if r == 0:
            lent = part.finished(part.more_acc[h])
            for u in range(shared):
                at = (h * shared + u) * HEAD_DIM
                att_ref[0, span:, at : at + HEAD_DIM] = lent[u * extra : (u + 1) * extra]

    with jax.named_scope("begin"):
        part.start()
    for i in range(pieces):
        fetch(i, block_of(i), path_sub(i)[1]).start()
    with jax.named_scope("prepare"):
        part.prepare()
    part.slots(0, 2, False)
    with jax.named_scope("pass_on"):
        part.pass_on(1, 0)
    with jax.named_scope("lent"):
        pl.when(middle)(lambda: part.lend().wait_recv())
        for h in range(kv_heads):
            part.attend(part.z, h, 0, 0, own=False, lent=True)
    part.slots(2, 6, True)
    chip = part.chip_of(3)
    with jax.named_scope("pass_on"):
        part.pass_on(jnp.where(middle, 0, 3), 1)
    part.look(chip)
    for h in range(kv_heads):
        with jax.named_scope("arrive"):
            part.arrived(h, chip, 1 - part.core)
        with jax.named_scope("attend_0"):
            part.turn(chip * CORES, CORES, h)
            part.attend(chip, h, 0, span, lent=True)
        with jax.named_scope("norm"):
            normalise(0, h)
    with jax.named_scope("first_0"):
        fetched(0)
        first_far(0)
        first_near(0)
    with jax.named_scope("attend_1"):
        for h in range(kv_heads):
            part.attend(chip, h, span, span)
            normalise(1, h)
    with jax.named_scope("first_1_far"):
        first_far(1)
        fetched(1)
    with jax.named_scope("second_0"):
        second(0)
    with jax.named_scope("first_1_near"):
        first_near(1)
    with jax.named_scope("third_0"):
        third(0)
    with jax.named_scope("second_1"):
        second(1)
    with jax.named_scope("third_1"):
        third(1)
    with jax.named_scope("add_0"):
        add_first(0)
    with jax.named_scope("last_0"):
        last(0)
        pl.when(middle)(lambda: give_back().start())
    with jax.named_scope("add_1"):
        add_first(1)
    with jax.named_scope("last_1"):
        last(1)
    with jax.named_scope("drain"):
        @pl.when(middle)
        def _():
            give_back().wait_send()

        @pl.when(jnp.logical_not(middle))
        def _():
            give_back().wait_recv()
            out_ref[kept:span] = back_in[...]
            part.lend().wait_send()

        for r in range(spans):
            sent(r)
        part.drain()


def fused(queries, keys, values, out_weight, span_order, document, n_ctx, kv_heads, first_of):
    slots = span_order.shape[0]
    span = document.shape[0] // slots
    rows, depth = queries.shape
    features = out_weight.shape[1]
    width = features // 16
    spans = rows // span
    heads = depth // HEAD_DIM
    extra = HEAD_DIM * kv_heads // heads
    most = span + extra
    f32, bf16 = jnp.float32, jnp.bfloat16
    hbm = pl.BlockSpec(memory_space=pl.ANY)
    vmem = pl.BlockSpec(memory_space=pltpu.VMEM)
    return pl.pallas_call(
        functools.partial(fused_kernel, n_ctx, kv_heads, first_of),
        out_shape=pltpu.VMEM((rows, features // 4), bf16),
        in_specs=[hbm] * 6,
        out_specs=vmem,
        scratch_shapes=[
            pltpu.VMEM((spans, most, depth), bf16),
            pltpu.VMEM((16, depth, width), bf16),
            pltpu.VMEM((spans, 12, most, width), bf16),
            pltpu.VMEM((spans, 12, most, width), bf16),
            pltpu.VMEM((spans, 4, most, width), f32),
            pltpu.VMEM((extra, features // 4), bf16),
            pltpu.VMEM((extra, features // 4), bf16),
            pltpu.SemaphoreType.DMA((2,)),
            pltpu.SemaphoreType.DMA((spans,)),
            pltpu.SemaphoreType.DMA((spans, 4)),
            pltpu.SemaphoreType.DMA((spans,)),
            pltpu.SemaphoreType.DMA((spans, 4)),
            pltpu.SemaphoreType.DMA((2,)),
        ]
        + attention_scratch(n_ctx, slots, rows, heads, kv_heads, span)
        + [
            pltpu.VMEM((extra, depth), bf16),
            pltpu.VMEM((kv_heads, HEAD_DIM, HEAD_DIM), bf16),
            pltpu.VMEM((8, span), jnp.int32),
            pltpu.VMEM((CORES * rows, HEAD_DIM), f32),
            pltpu.VMEM((kv_heads, 1, HEAD_DIM), f32),
            pltpu.VMEM((kv_heads, HEAD_DIM + ONES, HEAD_DIM), f32),
            pltpu.SemaphoreType.DMA((3,)),
        ],
        compiler_params=pltpu.CompilerParams(
            collective_id=0, has_side_effects=True, vmem_limit_bytes=60 * 1024 * 1024
        ),
        name="attend_project",
    )(span_order, document.reshape(slots, 1, span), queries, keys, values, out_weight)


def gather_attend(queries, keys, values, span_order, document, n_ctx, kv_heads, first_of):
    slots = span_order.shape[0]
    span = document.shape[0] // slots
    rows, depth = queries.shape
    hbm = pl.BlockSpec(memory_space=pl.ANY)
    vmem = pl.BlockSpec(memory_space=pltpu.VMEM)
    return pl.pallas_call(
        functools.partial(gather_attend_kernel, n_ctx, kv_heads, first_of),
        out_shape=jax.ShapeDtypeStruct(queries.shape, queries.dtype),
        in_specs=[hbm] * 5,
        out_specs=vmem,
        scratch_shapes=attention_scratch(n_ctx, slots, rows, depth // HEAD_DIM, kv_heads, span),
        compiler_params=pltpu.CompilerParams(collective_id=0, has_side_effects=True),
        name="gather_attend",
    )(span_order, document.reshape(slots, 1, span), queries, keys, values)


def shards(n_ctx, n_grp, queries, keys, values, out_weight, span_order, document):
    local_heads = queries.shape[1] // HEAD_DIM
    kv_heads = max(1, local_heads // QUERY_GROUP)

    def first_of(group):
        return group * local_heads // QUERY_GROUP

    spans = queries.shape[0] * span_order.shape[0] // document.shape[0]
    if n_grp == 4 and n_ctx == 4 * CORES and kv_heads == 2 and spans == 2:
        return fused(
            queries, keys, values, out_weight, span_order, document, n_ctx, kv_heads, first_of
        )
    attended = gather_attend(
        queries, keys, values, span_order, document, n_ctx, kv_heads, first_of
    )
    partial_value = jnp.dot(attended, out_weight, preferred_element_type=jnp.float32)
    return lax.psum_scatter(
        partial_value.astype(jnp.bfloat16), "grp", scatter_dimension=1, tiled=True
    )


def solution(mesh):
    in_specs = (P("ctx", "grp"), P("ctx", None), P("ctx", None), P("grp", None), P(), P())
    body = functools.partial(shards, mesh.shape["ctx"], mesh.shape["grp"])
    return jax.shard_map(
        body, mesh=mesh, in_specs=in_specs, out_specs=P("ctx", "grp"), check_vma=False
    )
```

```python
import functools
import math
from types import SimpleNamespace

import jax
import jax.numpy as jnp
from jax import lax
from jax.experimental import pallas as pl
from jax.experimental.pallas import tpu as pltpu
from jax.sharding import PartitionSpec as P

HEAD_DIM = 128
QUERY_GROUP = 8
CORES = 2
MESH = pl.DeviceIdType.MESH
HIDDEN = -1e30
ONES = 16


def attention(
    n_ctx, kv_heads, first_of, greeted, order_hbm, doc_hbm, q_hbm, k_hbm, v_hbm,
    order_ref, doc_rows, q_ref, kv_all, turned_ref, doc_cols, bias_ref, max_ref, acc_ref,
    local_sem, send_sem, recv_sem,
    few_q=None, more_q=None, more_doc=None, more_bias=None, more_max=None, more_acc=None,
    more_sem=None,
):
    nz = n_ctx // CORES
    me = lax.axis_index("ctx")
    group = lax.axis_index("grp")
    z, core = me // CORES, me % CORES
    partner = z * CORES + 1 - core
    tok_rows = kv_all.shape[2]
    span = doc_rows.shape[2]
    spans = tok_rows // span
    shared = q_ref.shape[1] // HEAD_DIM // kv_heads
    factor = math.log2(math.e) / math.sqrt(HEAD_DIM)
    keys_per_step = CORES * tok_rows
    near = jnp.minimum(z, nz - 1 - z)
    extra = HEAD_DIM // shared
    kept = span - extra
    mate = (z + 1 - 2 * (z % 2)) * CORES + core
    long_way = jnp.where(z < nz - 1 - z, 1, -1)

    def piece(way, h, chip, target):
        block = chip * CORES + core
        return pltpu.make_async_remote_copy(
            src_ref=kv_all.at[block, h],
            dst_ref=kv_all.at[block, h],
            send_sem=send_sem.at[way // 2],
            recv_sem=recv_sem.at[h, block],
            device_id=(target, group),
            device_id_type=MESH,
        )

    def arrived(h, chip, from_core):
        block = chip * CORES + from_core
        pltpu.make_async_copy(
            kv_all.at[block, h], kv_all.at[block, h], recv_sem.at[h, block]
        ).wait()

    def load(h, side):
        start = pl.multiple_of((first_of(group) + h) * HEAD_DIM, HEAD_DIM)
        return pltpu.make_async_copy(
            (k_hbm, v_hbm)[side].at[:, pl.ds(start, HEAD_DIM)],
            kv_all.at[me, h, :, pl.ds(side * HEAD_DIM, HEAD_DIM)],
            local_sem.at[h],
        )

    def loaded(h):
        pltpu.make_async_copy(kv_all.at[me, h], kv_all.at[me, h], local_sem.at[h]).wait()

    q_load = pltpu.make_async_copy(q_hbm, q_ref, local_sem.at[kv_heads])
    order_load = pltpu.make_async_copy(order_hbm, order_ref, local_sem.at[kv_heads + 1])
    doc_load = pltpu.make_async_copy(doc_hbm, doc_rows, local_sem.at[kv_heads + 2])

    def lend():
        return pltpu.make_async_remote_copy(
            src_ref=more_q,
            dst_ref=more_q,
            send_sem=more_sem.at[0],
            recv_sem=more_sem.at[1],
            device_id=(mate, group),
            device_id_type=MESH,
        )

    few_load = (
        None if more_q is None else
        pltpu.make_async_copy(q_hbm.at[pl.ds(kept, extra)], few_q, more_sem.at[2])
    )

    def stage():
        for head in range(kv_heads * shared):
            h, u = head // shared, head % shared
            more_q[h, u * extra : (u + 1) * extra] = few_q[
                :, head * HEAD_DIM : (head + 1) * HEAD_DIM
            ]
        lend().start()

    def start():
        for h in range(kv_heads):
            for side in range(2):
                load(h, side).start()
        order_load.start()
        doc_load.start()
        if few_load is not None:
            few_load.start()
        q_load.start()
        barrier = pltpu.get_barrier_semaphore()
        for target in [(partner, group)] + greeted:
            pl.semaphore_signal(barrier, inc=1, device_id=target, device_id_type=MESH)

        @pl.when(z > 0)
        def _():
            pl.semaphore_signal(
                barrier, inc=1, device_id=(me - CORES, group), device_id_type=MESH
            )

        @pl.when(z < nz - 1)
        def _():
            pl.semaphore_signal(
                barrier, inc=1, device_id=(me + CORES, group), device_id_type=MESH
            )

        pl.semaphore_wait(
            barrier, 1 + len(greeted) + jnp.minimum(z, 1) + jnp.minimum(nz - 1 - z, 1)
        )
        for h in range(kv_heads):
            loaded(h)

            @pl.when(z < nz - 1)
            def _():
                piece(0, h, z, me + CORES).start()

            @pl.when(z > 0)
            def _():
                piece(1, h, z, me - CORES).start()

            piece(2, h, z, partner).start()
            if h == 0 and few_load is not None:
                few_load.wait()
                pl.when(near == 0)(stage)

    def prepare():
        max_ref[...] = jnp.full(max_ref.shape, HIDDEN, jnp.float32)
        acc_ref[...] = jnp.zeros(acc_ref.shape, jnp.float32)
        order_load.wait()
        doc_load.wait()
        turned_ref[:, HEAD_DIM:] = jnp.ones(
            (turned_ref.shape[0], ONES, keys_per_step), turned_ref.dtype
        )
        for at in range(doc_rows.shape[0]):
            doc_cols[at] = jnp.transpose(jnp.broadcast_to(doc_rows[at], (span, span)))
        if more_q is not None:
            more_max[...] = jnp.full(more_max.shape, HIDDEN, jnp.float32)
            more_acc[...] = jnp.zeros(more_acc.shape, jnp.float32)
            theirs = jnp.broadcast_to(doc_rows[lent_span()], more_doc.shape)
            lane = lax.broadcasted_iota(jnp.int32, more_doc.shape, 1)
            rolled = theirs
            for u in range(shared):
                moved = pltpu.roll(theirs, (u * extra - kept) % span, 1)
                rolled = jnp.where(lane // extra == u, moved, rolled)
            more_doc[...] = rolled
        q_load.wait()

    def pass_on(n, h):
        def from_below():
            arrived(h, z - n, core)

            @pl.when(z < nz - 1)
            def _():
                piece(0, h, z - n, me + CORES).start()

            piece(2, h, z - n, partner).start()

        def from_above():
            arrived(h, z + n, core)

            @pl.when(z > 0)
            def _():
                piece(1, h, z + n, me - CORES).start()

            piece(2, h, z + n, partner).start()

        above_first = z < nz - 1 - z
        pl.when((n > 0) & (z + n < nz) & above_first)(from_above)
        pl.when((n > 0) & (z - n >= 0))(from_below)
        pl.when((n > 0) & (z + n < nz) & jnp.logical_not(above_first))(from_above)

    def chip_of(n):
        away = (n + 1) // 2
        paired = z + away * (1 - 2 * (n % 2))
        return jnp.where(n <= 2 * near, paired, z + long_way * (n - near))

    def lent_span():
        return order_ref[jnp.where(near == 1, mate, me) * spans]

    def look(chip):
        key_at = lax.broadcasted_iota(jnp.int32, (span, span), 0)
        row_at = lax.broadcasted_iota(jnp.int32, (span, span), 1)
        for slot in range(spans * CORES):
            key_span = order_ref[chip * (spans * CORES) + slot]
            key_doc = doc_cols[key_span]
            for r in range(spans):
                mine = order_ref[me * spans + r]
                seen = (key_doc == doc_rows[mine]) & (
                    key_span * span + key_at <= mine * span + row_at
                )
                bias_ref[slot * span : (slot + 1) * span, r * span : (r + 1) * span] = jnp.where(
                    seen, 0.0, HIDDEN
                )
            if more_q is not None:
                seen = (key_doc == more_doc[:1]) & (
                    key_span * span + key_at <= lent_span() * span + kept + row_at % extra
                )
                more_bias[slot * span : (slot + 1) * span] = jnp.where(seen, 0.0, HIDDEN)

    def keys_at(block, blocks):
        if blocks == CORES:
            return slice(None)
        return pl.ds(pl.multiple_of(block % CORES * tok_rows, tok_rows), blocks * tok_rows)

    def turn(block, blocks, h, spare=0):
        both = kv_all[pl.ds(block, blocks), h].reshape(blocks * tok_rows, 2 * HEAD_DIM)
        turned_ref[h + spare, :HEAD_DIM, keys_at(block, blocks)] = jnp.transpose(both[:, HEAD_DIM:])

    def attend(block, blocks, h, low, count, own=True, lent=False, spare=0):
        rows = pl.ds(low, count)
        keys = keys_at(block, blocks)
        key = kv_all[pl.ds(block, blocks), h].reshape(blocks * tok_rows, 2 * HEAD_DIM)
        key = key[:, :HEAD_DIM]
        asked = []
        if own:
            for u in range(shared):
                head = h * shared + u
                at = pl.ds(pl.multiple_of(head * HEAD_DIM, HEAD_DIM), HEAD_DIM)
                asked.append(
                    (q_ref[rows, at], bias_ref, max_ref.at[head], acc_ref.at[head], rows)
                )
        if lent:
            every = slice(None)
            asked.append((more_q[h], more_bias, more_max.at[h], more_acc.at[h], every))
        scores = [
            lax.dot_general(
                key, query, (((1,), (1,)), ((), ())), preferred_element_type=jnp.float32
            )
            + bias[keys, at]
            for query, bias, _, _, at in asked
        ]
        for (_, _, maxes, sums, at), score in zip(asked, scores):
            old = maxes[:, at]
            top = jnp.maximum(old, jnp.max(score, axis=0, keepdims=True))
            rescale = jnp.exp2((old - top) * factor)
            probs = jnp.exp2((score - top) * factor).astype(jnp.bfloat16)
            mixed = jnp.dot(
                turned_ref[h + spare, :, keys], probs, preferred_element_type=jnp.float32
            )
            maxes[:, at] = top
            sums[:, at] = sums[:, at] * rescale + mixed

    def plan(k):
        middle = near == 1
        after = k - 2
        first_n = jnp.where(middle, 2 * (after >= 2), 1 * (after == 0))
        first_h = jnp.where(middle, 1 * (after == 3), 1)
        second_n = jnp.where(middle, 1 * (after == 0), (after > 0) * (k + 1) // 2)
        second_h = jnp.where(middle, 1, (k + 1) % 2)
        chip = jnp.where(
            middle & (after >= 0), chip_of(1 + after % 2), chip_of(k // kv_heads)
        )
        held = jnp.where(middle & (after >= 0), after // 2, k % kv_heads)
        return first_n, first_h, second_n, second_h, chip, held

    def catch_up():
        lend().wait_recv()
        attend(chip_of(1) * CORES, CORES, 0, 0, 0, own=False, lent=True)
        look(z)
        for h in range(kv_heads):
            attend(z * CORES, CORES, h, 0, 0, own=False, lent=True, spare=kv_heads)

    def slots(begin, stop, lent):
        def one(k, carry):
            first_n, first_h, second_n, second_h, chip, held = plan(k)
            with jax.named_scope("pass_on"):
                if not lent:
                    pass_on(1 * (k == 2), 0)
                pass_on(first_n, first_h)
            look(chip)
            with jax.named_scope("arrive"):
                arrived(held, chip, 1 - core)
            spare = 0 if lent else jnp.where(k < 2, kv_heads, 0)
            turn(chip * CORES, CORES, held, spare)
            with jax.named_scope("attend"):
                attend(chip * CORES, CORES, held, 0, tok_rows, lent=lent, spare=spare)
            with jax.named_scope("pass_on"):
                pass_on(second_n, second_h)
            return carry

        lax.fori_loop(begin, stop, one, 0)

    def steps():
        def one(k, carry):
            n, h = k // kv_heads, k % kv_heads
            pass_on(n, h)
            look(chip_of(n))
            arrived(h, chip_of(n), 1 - core)
            turn(chip_of(n) * CORES, CORES, h)
            attend(chip_of(n) * CORES, CORES, h, 0, tok_rows)
            return carry

        lax.fori_loop(0, nz * kv_heads, one, 0)

    def finished(total):
        scale = 1.0 / total[HEAD_DIM : HEAD_DIM + 1]
        return jnp.transpose((total[:HEAD_DIM] * scale).astype(jnp.bfloat16))

    def result(head, low, count):
        return finished(acc_ref[head, :, pl.ds(low, count)])

    def drain():
        pltpu.make_async_copy(kv_all.at[:nz], kv_all.at[:nz], send_sem.at[1]).wait()
        for at in range(nz):
            sent = (at + 1) * (at < nz - 1) + (nz - at) * (at > 0)

            @pl.when(z == at)
            def _():
                blocks = kv_all.at[:sent]
                pltpu.make_async_copy(blocks, blocks, send_sem.at[0]).wait()

    return SimpleNamespace(**locals())


def attention_scratch(n_ctx, slots, rows, heads, kv_heads, span):
    f32, bf16 = jnp.float32, jnp.bfloat16
    return [
        pltpu.SMEM((slots,), jnp.int32),
        pltpu.VMEM((slots, 1, span), jnp.int32),
        pltpu.VMEM((rows, heads * HEAD_DIM), bf16),
        pltpu.VMEM((n_ctx, kv_heads, rows, 2 * HEAD_DIM), bf16),
        pltpu.VMEM((2 * kv_heads, HEAD_DIM + ONES, CORES * rows), bf16),
        pltpu.VMEM((slots, span, span), jnp.int32),
        pltpu.VMEM((CORES * rows, rows), f32),
        pltpu.VMEM((heads, 1, rows), f32),
        pltpu.VMEM((heads, HEAD_DIM + ONES, rows), f32),
        pltpu.SemaphoreType.DMA((kv_heads + 3,)),
        pltpu.SemaphoreType.DMA((2,)),
        pltpu.SemaphoreType.DMA((kv_heads, n_ctx)),
    ]


def gather_attend_kernel(
    n_ctx, kv_heads, first_of, order_hbm, doc_hbm, q_hbm, k_hbm, v_hbm, out_ref, *scratch
):
    part = attention(
        n_ctx, kv_heads, first_of, [], order_hbm, doc_hbm, q_hbm, k_hbm, v_hbm, *scratch
    )
    part.start()
    part.prepare()
    part.steps()
    rows, width = out_ref.shape
    for head in range(width // HEAD_DIM):
        out_ref[:, head * HEAD_DIM : (head + 1) * HEAD_DIM] = part.result(head, 0, rows)
    part.drain()


def fused_kernel(
    n_ctx, kv_heads, first_of, order_hbm, doc_hbm, q_hbm, k_hbm, v_hbm, w_hbm, out_ref,
    att_ref, w_buf, send_ref, got_ref, own_ref, back_out, back_in,
    w_sem, sent_sem, far_sem, near_sem, two_sem, back_sem, *scratch,
):
    me = lax.axis_index("ctx")
    group = lax.axis_index("grp")
    side = group + 1 - 2 * (group % 2)
    other = (group + 2) % 4
    far = 3 - group
    pieces, _, width = w_buf.shape
    block_width = out_ref.shape[1]
    part = attention(
        n_ctx, kv_heads, first_of, [(me, side), (me, other)],
        order_hbm, doc_hbm, q_hbm, k_hbm, v_hbm, *scratch,
    )
    span, spans, extra, kept, shared = part.span, part.spans, part.extra, part.kept, part.shared
    middle = part.near == 1

    def path_sub(i):
        path = i % 2
        return path, 2 * path + (i // 2) % 2

    def block_of(i):
        path = i % 2
        first = far if i < 4 else (other if path else side)
        return first if i < 8 else ((side if path else other) if i < 12 else group)

    def fetch(i, block, sub):
        start = pl.multiple_of(block * block_width + sub * width, width)
        return pltpu.make_async_copy(
            w_hbm.at[:, pl.ds(start, width)], w_buf.at[i], w_sem.at[i // 8]
        )

    def fetched(half):
        part_of = w_buf.at[pl.ds(half * 8, 8)]
        pltpu.make_async_copy(part_of, part_of, w_sem.at[half]).wait()

    def held_rows(r):
        return span if r else span + extra

    def sized(r, do):
        if r:
            do(span)
        else:
            pl.when(middle)(lambda: do(span + extra))
            pl.when(jnp.logical_not(middle))(lambda: do(kept))

    def product(r, i):
        return jnp.dot(
            att_ref[r, : held_rows(r)], w_buf[i], preferred_element_type=jnp.float32
        )

    def send(r, i, path, sem):
        sized(
            r,
            lambda count: pltpu.make_async_remote_copy(
                src_ref=send_ref.at[r, i, :count],
                dst_ref=got_ref.at[r, i, :count],
                send_sem=sent_sem.at[r],
                recv_sem=sem,
                device_id=(me, (1 - path) * side + path * other),
                device_id_type=MESH,
            ).start(),
        )

    def got(r, low, pieces_of, sem):
        def wait(count):
            part_of = got_ref.at[r, pl.ds(low, pieces_of), :count]
            pltpu.make_async_copy(part_of, part_of, sem).wait()

        sized(r, wait)

    def sent(r):
        def wait(count):
            part_of = send_ref.at[r, :, :count]
            pltpu.make_async_copy(part_of, part_of, sent_sem.at[r]).wait()

        sized(r, wait)

    def give_back():
        return pltpu.make_async_remote_copy(
            src_ref=back_out,
            dst_ref=back_in,
            send_sem=back_sem.at[0],
            recv_sem=back_sem.at[1],
            device_id=(part.mate, group),
            device_id_type=MESH,
        )

    def swapped(i):
        return jnp.where(part.core == 1, i + 1 - 2 * (i % 2), i)

    def first_far(r):
        def one(at, carry):
            i = swapped(at)
            send_ref[r, i, : held_rows(r)] = product(r, i).astype(send_ref.dtype)
            send(r, i, i % 2, far_sem.at[r, i])
            return carry

        lax.fori_loop(0, 4, one, 0)

    def first_near(r):
        def one(at, carry):
            i = swapped(at)
            send_ref[r, i, : held_rows(r)] = product(r, i).astype(send_ref.dtype)
            send(r, i, i % 2, near_sem.at[r])
            return carry

        lax.fori_loop(4, 8, one, 0)

    def second(r):
        def one(at, carry):
            i = swapped(at)
            value = product(r, i)
            got(r, i - 8, 1, far_sem.at[r, i - 8])
            count = held_rows(r)
            send_ref[r, i, :count] = (
                value + got_ref[r, i - 8, :count].astype(jnp.float32)
            ).astype(send_ref.dtype)
            send(r, i, 1 - i % 2, two_sem.at[r, i - 8])
            return carry

        lax.fori_loop(8, 12, one, 0)

    def third(r):
        def one(j, carry):
            own_ref[r, j, : held_rows(r)] = product(r, 12 + j)
            return carry

        lax.fori_loop(0, 4, one, 0)

    def add_first(r):
        got(r, 4, 4, near_sem.at[r])
        for j in range(4):
            count = held_rows(r)
            own_ref[r, j, :count] = own_ref[r, j, :count] + got_ref[r, 4 + j, :count].astype(
                jnp.float32
            )

    def last(r):
        for j in range(4):
            got(r, 8 + j, 1, two_sem.at[r, j])
            at = path_sub(j)[1] * width
            total = (
                own_ref[r, j, : held_rows(r)]
                + got_ref[r, 8 + j, : held_rows(r)].astype(jnp.float32)
            ).astype(out_ref.dtype)
            if r:
                out_ref[span:, at : at + width] = total
            else:
                out_ref[:kept, at : at + width] = total[:kept]

                @pl.when(middle)
                def _():
                    out_ref[kept:span, at : at + width] = total[kept:span]
                    back_out[:, at : at + width] = total[span:]

    def normalise(r, h):
        for head in range(h * shared, (h + 1) * shared):
            att_ref[r, :span, head * HEAD_DIM : (head + 1) * HEAD_DIM] = part.result(
                head, r * span, span
            )
        if r == 0:
            lent = part.finished(part.more_acc[h])
            for u in range(shared):
                at = (h * shared + u) * HEAD_DIM
                att_ref[0, span:, at : at + HEAD_DIM] = lent[u * extra : (u + 1) * extra]

    with jax.named_scope("begin"):
        part.start()
    for i in range(pieces):
        fetch(i, block_of(i), path_sub(i)[1]).start()
    with jax.named_scope("prepare"):
        part.prepare()
    part.slots(0, 3, False)
    with jax.named_scope("lent"):
        pl.when(middle)(part.catch_up)
    part.slots(3, 6, True)
    chip = part.chip_of(3)
    part.look(chip)
    block, own, partners = (
        chip * CORES, chip * CORES + part.core, chip * CORES + 1 - part.core
    )

    def whole(h):
        part.arrived(h, chip, 1 - part.core)
        part.turn(block, CORES, h)
        part.attend(block, CORES, h, 0, span, lent=True)

    def halves(h):
        if h:
            with jax.named_scope("pass_on"):
                part.pass_on(3, h)
        with jax.named_scope("own_half"):
            part.turn(own, 1, h)
            part.attend(own, 1, h, 0, span)
        with jax.named_scope("arrive"):
            part.arrived(h, chip, 1 - part.core)
        with jax.named_scope("other_half"):
            part.turn(partners, 1, h)
            part.attend(partners, 1, h, 0, span)

    for h in range(kv_heads):
        with jax.named_scope("attend_0"):
            pl.when(middle)(functools.partial(whole, h))
            pl.when(jnp.logical_not(middle))(functools.partial(halves, h))
        with jax.named_scope("norm"):
            normalise(0, h)
    with jax.named_scope("first_0"):
        fetched(0)
        first_far(0)
        first_near(0)
    with jax.named_scope("attend_1"):
        for h in range(kv_heads):
            part.attend(block, CORES, h, span, span)
            normalise(1, h)
    with jax.named_scope("first_1_far"):
        first_far(1)
        fetched(1)
    with jax.named_scope("second_0"):
        second(0)
    with jax.named_scope("first_1_near"):
        first_near(1)
    with jax.named_scope("third_0"):
        third(0)
    with jax.named_scope("second_1"):
        second(1)
    with jax.named_scope("third_1"):
        third(1)
    with jax.named_scope("add_0"):
        add_first(0)
    with jax.named_scope("last_0"):
        last(0)
        pl.when(middle)(lambda: give_back().start())
    with jax.named_scope("add_1"):
        add_first(1)
    with jax.named_scope("last_1"):
        last(1)
    with jax.named_scope("drain"):
        @pl.when(middle)
        def _():
            give_back().wait_send()

        @pl.when(jnp.logical_not(middle))
        def _():
            give_back().wait_recv()
            out_ref[kept:span] = back_in[...]
            part.lend().wait_send()

        for r in range(spans):
            sent(r)
        part.drain()


def fused(queries, keys, values, out_weight, span_order, document, n_ctx, kv_heads, first_of):
    slots = span_order.shape[0]
    span = document.shape[0] // slots
    rows, depth = queries.shape
    features = out_weight.shape[1]
    width = features // 16
    spans = rows // span
    heads = depth // HEAD_DIM
    extra = HEAD_DIM * kv_heads // heads
    most = span + extra
    f32, bf16 = jnp.float32, jnp.bfloat16
    hbm = pl.BlockSpec(memory_space=pl.ANY)
    vmem = pl.BlockSpec(memory_space=pltpu.VMEM)
    return pl.pallas_call(
        functools.partial(fused_kernel, n_ctx, kv_heads, first_of),
        out_shape=pltpu.VMEM((rows, features // 4), bf16),
        in_specs=[hbm] * 6,
        out_specs=vmem,
        scratch_shapes=[
            pltpu.VMEM((spans, most, depth), bf16),
            pltpu.VMEM((16, depth, width), bf16),
            pltpu.VMEM((spans, 12, most, width), bf16),
            pltpu.VMEM((spans, 12, most, width), bf16),
            pltpu.VMEM((spans, 4, most, width), f32),
            pltpu.VMEM((extra, features // 4), bf16),
            pltpu.VMEM((extra, features // 4), bf16),
            pltpu.SemaphoreType.DMA((2,)),
            pltpu.SemaphoreType.DMA((spans,)),
            pltpu.SemaphoreType.DMA((spans, 4)),
            pltpu.SemaphoreType.DMA((spans,)),
            pltpu.SemaphoreType.DMA((spans, 4)),
            pltpu.SemaphoreType.DMA((2,)),
        ]
        + attention_scratch(n_ctx, slots, rows, heads, kv_heads, span)
        + [
            pltpu.VMEM((extra, depth), bf16),
            pltpu.VMEM((kv_heads, HEAD_DIM, HEAD_DIM), bf16),
            pltpu.VMEM((8, span), jnp.int32),
            pltpu.VMEM((CORES * rows, HEAD_DIM), f32),
            pltpu.VMEM((kv_heads, 1, HEAD_DIM), f32),
            pltpu.VMEM((kv_heads, HEAD_DIM + ONES, HEAD_DIM), f32),
            pltpu.SemaphoreType.DMA((3,)),
        ],
        compiler_params=pltpu.CompilerParams(
            collective_id=0, has_side_effects=True, vmem_limit_bytes=60 * 1024 * 1024
        ),
        name="attend_project",
    )(span_order, document.reshape(slots, 1, span), queries, keys, values, out_weight)


def gather_attend(queries, keys, values, span_order, document, n_ctx, kv_heads, first_of):
    slots = span_order.shape[0]
    span = document.shape[0] // slots
    rows, depth = queries.shape
    hbm = pl.BlockSpec(memory_space=pl.ANY)
    vmem = pl.BlockSpec(memory_space=pltpu.VMEM)
    return pl.pallas_call(
        functools.partial(gather_attend_kernel, n_ctx, kv_heads, first_of),
        out_shape=jax.ShapeDtypeStruct(queries.shape, queries.dtype),
        in_specs=[hbm] * 5,
        out_specs=vmem,
        scratch_shapes=attention_scratch(n_ctx, slots, rows, depth // HEAD_DIM, kv_heads, span),
        compiler_params=pltpu.CompilerParams(collective_id=0, has_side_effects=True),
        name="gather_attend",
    )(span_order, document.reshape(slots, 1, span), queries, keys, values)


def shards(n_ctx, n_grp, queries, keys, values, out_weight, span_order, document):
    local_heads = queries.shape[1] // HEAD_DIM
    kv_heads = max(1, local_heads // QUERY_GROUP)

    def first_of(group):
        return group * local_heads // QUERY_GROUP

    spans = queries.shape[0] * span_order.shape[0] // document.shape[0]
    if n_grp == 4 and n_ctx == 4 * CORES and kv_heads == 2 and spans == 2:
        return fused(
            queries, keys, values, out_weight, span_order, document, n_ctx, kv_heads, first_of
        )
    attended = gather_attend(
        queries, keys, values, span_order, document, n_ctx, kv_heads, first_of
    )
    partial_value = jnp.dot(attended, out_weight, preferred_element_type=jnp.float32)
    return lax.psum_scatter(
        partial_value.astype(jnp.bfloat16), "grp", scatter_dimension=1, tiled=True
    )


def solution(mesh):
    in_specs = (P("ctx", "grp"), P("ctx", None), P("ctx", None), P("grp", None), P(), P())
    body = functools.partial(shards, mesh.shape["ctx"], mesh.shape["grp"])
    return jax.shard_map(
        body, mesh=mesh, in_specs=in_specs, out_specs=P("ctx", "grp"), check_vma=False
    )
```

```python
import functools
import math
from types import SimpleNamespace

import jax
import jax.numpy as jnp
from jax import lax
from jax.experimental import pallas as pl
from jax.experimental.pallas import tpu as pltpu
from jax.sharding import PartitionSpec as P

HEAD_DIM = 128
QUERY_GROUP = 8
CORES = 2
MESH = pl.DeviceIdType.MESH
HIDDEN = -1e30
ONES = 16


def attention(
    n_ctx, kv_heads, first_of, greeted, order_hbm, doc_hbm, q_hbm, k_hbm, v_hbm,
    order_ref, doc_rows, q_ref, kv_all, turned_ref, doc_cols, bias_ref, max_ref, acc_ref,
    local_sem, send_sem, recv_sem,
    few_q=None, more_q=None, more_doc=None, more_bias=None, more_max=None, more_acc=None,
    more_sem=None,
):
    nz = n_ctx // CORES
    me = lax.axis_index("ctx")
    group = lax.axis_index("grp")
    z, core = me // CORES, me % CORES
    partner = z * CORES + 1 - core
    tok_rows = kv_all.shape[2]
    span = doc_rows.shape[2]
    spans = tok_rows // span
    shared = q_ref.shape[1] // HEAD_DIM // kv_heads
    factor = math.log2(math.e) / math.sqrt(HEAD_DIM)
    keys_per_step = CORES * tok_rows
    near = jnp.minimum(z, nz - 1 - z)
    extra = HEAD_DIM // shared
    kept = span - extra
    mate = (z + 1 - 2 * (z % 2)) * CORES + core
    long_way = jnp.where(z < nz - 1 - z, 1, -1)

    def piece(way, h, chip, target):
        block = chip * CORES + core
        return pltpu.make_async_remote_copy(
            src_ref=kv_all.at[block, h],
            dst_ref=kv_all.at[block, h],
            send_sem=send_sem.at[way // 2],
            recv_sem=recv_sem.at[h, block],
            device_id=(target, group),
            device_id_type=MESH,
        )

    def arrived(h, chip, from_core):
        block = chip * CORES + from_core
        pltpu.make_async_copy(
            kv_all.at[block, h], kv_all.at[block, h], recv_sem.at[h, block]
        ).wait()

    def load(h, side):
        start = pl.multiple_of((first_of(group) + h) * HEAD_DIM, HEAD_DIM)
        return pltpu.make_async_copy(
            (k_hbm, v_hbm)[side].at[:, pl.ds(start, HEAD_DIM)],
            kv_all.at[me, h, :, pl.ds(side * HEAD_DIM, HEAD_DIM)],
            local_sem.at[h],
        )

    def loaded(h):
        pltpu.make_async_copy(kv_all.at[me, h], kv_all.at[me, h], local_sem.at[h]).wait()

    q_load = pltpu.make_async_copy(q_hbm, q_ref, local_sem.at[kv_heads])
    order_load = pltpu.make_async_copy(order_hbm, order_ref, local_sem.at[kv_heads + 1])
    doc_load = pltpu.make_async_copy(doc_hbm, doc_rows, local_sem.at[kv_heads + 2])

    def lend():
        return pltpu.make_async_remote_copy(
            src_ref=more_q,
            dst_ref=more_q,
            send_sem=more_sem.at[0],
            recv_sem=more_sem.at[1],
            device_id=(mate, group),
            device_id_type=MESH,
        )

    few_load = (
        None if more_q is None else
        pltpu.make_async_copy(q_hbm.at[pl.ds(kept, extra)], few_q, more_sem.at[2])
    )

    def stage():
        for head in range(kv_heads * shared):
            h, u = head // shared, head % shared
            more_q[h, u * extra : (u + 1) * extra] = few_q[
                :, head * HEAD_DIM : (head + 1) * HEAD_DIM
            ]
        lend().start()

    def start():
        for h in range(kv_heads):
            for side in range(2):
                load(h, side).start()
        order_load.start()
        doc_load.start()
        if few_load is not None:
            few_load.start()
        q_load.start()
        barrier = pltpu.get_barrier_semaphore()
        for target in [(partner, group)] + greeted:
            pl.semaphore_signal(barrier, inc=1, device_id=target, device_id_type=MESH)

        @pl.when(z > 0)
        def _():
            pl.semaphore_signal(
                barrier, inc=1, device_id=(me - CORES, group), device_id_type=MESH
            )

        @pl.when(z < nz - 1)
        def _():
            pl.semaphore_signal(
                barrier, inc=1, device_id=(me + CORES, group), device_id_type=MESH
            )

        pl.semaphore_wait(
            barrier, 1 + len(greeted) + jnp.minimum(z, 1) + jnp.minimum(nz - 1 - z, 1)
        )
        for h in range(kv_heads):
            loaded(h)

            @pl.when(z < nz - 1)
            def _():
                piece(0, h, z, me + CORES).start()

            @pl.when(z > 0)
            def _():
                piece(1, h, z, me - CORES).start()

            piece(2, h, z, partner).start()
            if h == 0 and few_load is not None:
                few_load.wait()
                pl.when(near == 0)(stage)

    def prepare():
        max_ref[...] = jnp.full(max_ref.shape, HIDDEN, jnp.float32)
        acc_ref[...] = jnp.zeros(acc_ref.shape, jnp.float32)
        order_load.wait()
        doc_load.wait()
        turned_ref[:, HEAD_DIM:] = jnp.ones(
            (turned_ref.shape[0], ONES, keys_per_step), turned_ref.dtype
        )
        for at in range(doc_rows.shape[0]):
            doc_cols[at] = jnp.transpose(jnp.broadcast_to(doc_rows[at], (span, span)))
        if more_q is not None:
            more_max[...] = jnp.full(more_max.shape, HIDDEN, jnp.float32)
            more_acc[...] = jnp.zeros(more_acc.shape, jnp.float32)
            theirs = jnp.broadcast_to(doc_rows[lent_span()], more_doc.shape)
            lane = lax.broadcasted_iota(jnp.int32, more_doc.shape, 1)
            rolled = theirs
            for u in range(shared):
                moved = pltpu.roll(theirs, (u * extra - kept) % span, 1)
                rolled = jnp.where(lane // extra == u, moved, rolled)
            more_doc[...] = rolled
        q_load.wait()

    def pass_on(n, h):
        def from_below():
            arrived(h, z - n, core)

            @pl.when(z < nz - 1)
            def _():
                piece(0, h, z - n, me + CORES).start()

            piece(2, h, z - n, partner).start()

        def from_above():
            arrived(h, z + n, core)

            @pl.when(z > 0)
            def _():
                piece(1, h, z + n, me - CORES).start()

            piece(2, h, z + n, partner).start()

        above_first = z < nz - 1 - z
        pl.when((n > 0) & (z + n < nz) & above_first)(from_above)
        pl.when((n > 0) & (z - n >= 0))(from_below)
        pl.when((n > 0) & (z + n < nz) & jnp.logical_not(above_first))(from_above)

    def chip_of(n):
        away = (n + 1) // 2
        paired = z + away * (1 - 2 * (n % 2))
        return jnp.where(n <= 2 * near, paired, z + long_way * (n - near))

    def lent_span():
        return order_ref[jnp.where(near == 1, mate, me) * spans]

    def look(chip):
        key_at = lax.broadcasted_iota(jnp.int32, (span, span), 0)
        row_at = lax.broadcasted_iota(jnp.int32, (span, span), 1)
        for slot in range(spans * CORES):
            key_span = order_ref[chip * (spans * CORES) + slot]
            key_doc = doc_cols[key_span]
            for r in range(spans):
                mine = order_ref[me * spans + r]
                seen = (key_doc == doc_rows[mine]) & (
                    key_span * span + key_at <= mine * span + row_at
                )
                bias_ref[slot * span : (slot + 1) * span, r * span : (r + 1) * span] = jnp.where(
                    seen, 0.0, HIDDEN
                )
            if more_q is not None:
                seen = (key_doc == more_doc[:1]) & (
                    key_span * span + key_at <= lent_span() * span + kept + row_at % extra
                )
                more_bias[slot * span : (slot + 1) * span] = jnp.where(seen, 0.0, HIDDEN)

    def keys_at(block, blocks):
        if blocks == CORES:
            return slice(None)
        return pl.ds(pl.multiple_of(block % CORES * tok_rows, tok_rows), blocks * tok_rows)

    def turn(block, blocks, h, spare=0):
        both = kv_all[pl.ds(block, blocks), h].reshape(blocks * tok_rows, 2 * HEAD_DIM)
        turned_ref[h + spare, :HEAD_DIM, keys_at(block, blocks)] = jnp.transpose(both[:, HEAD_DIM:])

    def attend(block, blocks, h, low, count, own=True, lent=False, spare=0):
        rows = pl.ds(low, count)
        keys = keys_at(block, blocks)
        key = kv_all[pl.ds(block, blocks), h].reshape(blocks * tok_rows, 2 * HEAD_DIM)
        key = key[:, :HEAD_DIM]
        asked = []
        if own:
            for u in range(shared):
                head = h * shared + u
                at = pl.ds(pl.multiple_of(head * HEAD_DIM, HEAD_DIM), HEAD_DIM)
                asked.append(
                    (q_ref[rows, at], bias_ref, max_ref.at[head], acc_ref.at[head], rows)
                )
        if lent:
            every = slice(None)
            asked.append((more_q[h], more_bias, more_max.at[h], more_acc.at[h], every))
        scores = [
            lax.dot_general(
                key, query, (((1,), (1,)), ((), ())), preferred_element_type=jnp.float32
            )
            + bias[keys, at]
            for query, bias, _, _, at in asked
        ]
        for (_, _, maxes, sums, at), score in zip(asked, scores):
            old = maxes[:, at]
            top = jnp.maximum(old, jnp.max(score, axis=0, keepdims=True))
            rescale = jnp.exp2((old - top) * factor)
            probs = jnp.exp2((score - top) * factor).astype(jnp.bfloat16)
            mixed = jnp.dot(
                turned_ref[h + spare, :, keys], probs, preferred_element_type=jnp.float32
            )
            maxes[:, at] = top
            sums[:, at] = sums[:, at] * rescale + mixed

    def plan(k):
        middle = near == 1
        after = k - 2
        first_n = jnp.where(middle, 2 * (after >= 2), 1 * (after == 0))
        first_h = jnp.where(middle, 1 * (after == 3), 1)
        second_n = jnp.where(middle, 1 * (after == 0), (after > 0) * (k + 1) // 2)
        second_h = jnp.where(middle, 1, (k + 1) % 2)
        chip = jnp.where(
            middle & (after >= 0), chip_of(1 + after % 2), chip_of(k // kv_heads)
        )
        held = jnp.where(middle & (after >= 0), after // 2, k % kv_heads)
        return first_n, first_h, second_n, second_h, chip, held

    def catch_up():
        lend().wait_recv()
        attend(chip_of(1) * CORES, CORES, 0, 0, 0, own=False, lent=True)
        look(z)
        for h in range(kv_heads):
            attend(z * CORES, CORES, h, 0, 0, own=False, lent=True, spare=kv_heads)

    def slots(begin, stop, lent, count=None):
        def one(k, carry):
            first_n, first_h, second_n, second_h, chip, held = plan(k)
            with jax.named_scope("pass_on"):
                if not lent:
                    pass_on(1 * (k == 2), 0)
                pass_on(first_n, first_h)
            look(chip)
            with jax.named_scope("arrive"):
                arrived(held, chip, 1 - core)
            spare = 0 if lent else jnp.where(k < 2, kv_heads, 0)
            turn(chip * CORES, CORES, held, spare)
            with jax.named_scope("attend"):
                attend(
                    chip * CORES, CORES, held, 0, count or tok_rows, lent=lent, spare=spare
                )
            with jax.named_scope("pass_on"):
                pass_on(second_n, second_h)
            return carry

        lax.fori_loop(begin, stop, one, 0)

    def steps():
        def one(k, carry):
            n, h = k // kv_heads, k % kv_heads
            pass_on(n, h)
            look(chip_of(n))
            arrived(h, chip_of(n), 1 - core)
            turn(chip_of(n) * CORES, CORES, h)
            attend(chip_of(n) * CORES, CORES, h, 0, tok_rows)
            return carry

        lax.fori_loop(0, nz * kv_heads, one, 0)

    def finished(total):
        scale = 1.0 / total[HEAD_DIM : HEAD_DIM + 1]
        return jnp.transpose((total[:HEAD_DIM] * scale).astype(jnp.bfloat16))

    def result(head, low, count):
        return finished(acc_ref[head, :, pl.ds(low, count)])

    def drain():
        pltpu.make_async_copy(kv_all.at[:nz], kv_all.at[:nz], send_sem.at[1]).wait()
        for at in range(nz):
            sent = (at + 1) * (at < nz - 1) + (nz - at) * (at > 0)

            @pl.when(z == at)
            def _():
                blocks = kv_all.at[:sent]
                pltpu.make_async_copy(blocks, blocks, send_sem.at[0]).wait()

    return SimpleNamespace(**locals())


def attention_scratch(n_ctx, slots, rows, heads, kv_heads, span):
    f32, bf16 = jnp.float32, jnp.bfloat16
    return [
        pltpu.SMEM((slots,), jnp.int32),
        pltpu.VMEM((slots, 1, span), jnp.int32),
        pltpu.VMEM((rows, heads * HEAD_DIM), bf16),
        pltpu.VMEM((n_ctx, kv_heads, rows, 2 * HEAD_DIM), bf16),
        pltpu.VMEM((2 * kv_heads, HEAD_DIM + ONES, CORES * rows), bf16),
        pltpu.VMEM((slots, span, span), jnp.int32),
        pltpu.VMEM((CORES * rows, rows), f32),
        pltpu.VMEM((heads, 1, rows), f32),
        pltpu.VMEM((heads, HEAD_DIM + ONES, rows), f32),
        pltpu.SemaphoreType.DMA((kv_heads + 3,)),
        pltpu.SemaphoreType.DMA((2,)),
        pltpu.SemaphoreType.DMA((kv_heads, n_ctx)),
    ]


def gather_attend_kernel(
    n_ctx, kv_heads, first_of, order_hbm, doc_hbm, q_hbm, k_hbm, v_hbm, out_ref, *scratch
):
    part = attention(
        n_ctx, kv_heads, first_of, [], order_hbm, doc_hbm, q_hbm, k_hbm, v_hbm, *scratch
    )
    part.start()
    part.prepare()
    part.steps()
    rows, width = out_ref.shape
    for head in range(width // HEAD_DIM):
        out_ref[:, head * HEAD_DIM : (head + 1) * HEAD_DIM] = part.result(head, 0, rows)
    part.drain()


def fused_kernel(
    n_ctx, kv_heads, first_of, order_hbm, doc_hbm, q_hbm, k_hbm, v_hbm, w_hbm, out_ref,
    att_ref, w_buf, send_ref, got_ref, own_ref, back_out, back_in,
    w_sem, sent_sem, far_sem, near_sem, two_sem, back_sem, *scratch,
):
    me = lax.axis_index("ctx")
    group = lax.axis_index("grp")
    side = group + 1 - 2 * (group % 2)
    other = (group + 2) % 4
    far = 3 - group
    pieces, _, width = w_buf.shape
    block_width = out_ref.shape[1]
    part = attention(
        n_ctx, kv_heads, first_of, [(me, side), (me, other)],
        order_hbm, doc_hbm, q_hbm, k_hbm, v_hbm, *scratch,
    )
    span, spans, extra, kept, shared = part.span, part.spans, part.extra, part.kept, part.shared
    middle = part.near == 1

    def path_sub(i):
        path = i % 2
        return path, 2 * path + (i // 2) % 2

    def block_of(i):
        path = i % 2
        first = far if i < 4 else (other if path else side)
        return first if i < 8 else ((side if path else other) if i < 12 else group)

    def fetch(i, block, sub):
        start = pl.multiple_of(block * block_width + sub * width, width)
        return pltpu.make_async_copy(
            w_hbm.at[:, pl.ds(start, width)], w_buf.at[i], w_sem.at[i // 8]
        )

    def fetched(half):
        part_of = w_buf.at[pl.ds(half * 8, 8)]
        pltpu.make_async_copy(part_of, part_of, w_sem.at[half]).wait()

    def held_rows(r):
        return span if r else span + extra

    def sized(r, do):
        if r:
            do(span)
        else:
            pl.when(middle)(lambda: do(span + extra))
            pl.when(jnp.logical_not(middle))(lambda: do(kept))

    def product(r, i):
        return jnp.dot(
            att_ref[r, : held_rows(r)], w_buf[i], preferred_element_type=jnp.float32
        )

    def send(r, i, path, sem):
        sized(
            r,
            lambda count: pltpu.make_async_remote_copy(
                src_ref=send_ref.at[r, i, :count],
                dst_ref=got_ref.at[r, i, :count],
                send_sem=sent_sem.at[r],
                recv_sem=sem,
                device_id=(me, (1 - path) * side + path * other),
                device_id_type=MESH,
            ).start(),
        )

    def got(r, low, pieces_of, sem):
        def wait(count):
            part_of = got_ref.at[r, pl.ds(low, pieces_of), :count]
            pltpu.make_async_copy(part_of, part_of, sem).wait()

        sized(r, wait)

    def sent(r):
        def wait(count):
            part_of = send_ref.at[r, :, :count]
            pltpu.make_async_copy(part_of, part_of, sent_sem.at[r]).wait()

        sized(r, wait)

    def give_back():
        return pltpu.make_async_remote_copy(
            src_ref=back_out,
            dst_ref=back_in,
            send_sem=back_sem.at[0],
            recv_sem=back_sem.at[1],
            device_id=(part.mate, group),
            device_id_type=MESH,
        )

    def swapped(i):
        return jnp.where(part.core == 1, i + 1 - 2 * (i % 2), i)

    half = att_ref.shape[2] // 2

    def early_products():
        def one(i, carry):
            own_ref[1, i] = jnp.dot(
                att_ref[0, :, :half], w_buf[i, :half], preferred_element_type=jnp.float32
            )
            return carry

        lax.fori_loop(0, 2, one, 0)

    def late_products():
        def one(at, carry):
            i = swapped(at)
            rest = jnp.dot(
                att_ref[0, :, half:], w_buf[i, half:], preferred_element_type=jnp.float32
            )
            send_ref[0, i] = (own_ref[1, i] + rest).astype(send_ref.dtype)
            send(0, i, i % 2, far_sem.at[0, i])
            return carry

        lax.fori_loop(0, 2, one, 0)

    def first_far(r, low=0, high=4):
        def one(at, carry):
            i = swapped(at)
            send_ref[r, i, : held_rows(r)] = product(r, i).astype(send_ref.dtype)
            send(r, i, i % 2, far_sem.at[r, i])
            return carry

        lax.fori_loop(low, high, one, 0)

    def first_near(r):
        def one(at, carry):
            i = swapped(at)
            send_ref[r, i, : held_rows(r)] = product(r, i).astype(send_ref.dtype)
            send(r, i, i % 2, near_sem.at[r])
            return carry

        lax.fori_loop(4, 8, one, 0)

    def second(r):
        def one(at, carry):
            i = swapped(at)
            value = product(r, i)
            got(r, i - 8, 1, far_sem.at[r, i - 8])
            count = held_rows(r)
            send_ref[r, i, :count] = (
                value + got_ref[r, i - 8, :count].astype(jnp.float32)
            ).astype(send_ref.dtype)
            send(r, i, 1 - i % 2, two_sem.at[r, i - 8])
            return carry

        lax.fori_loop(8, 12, one, 0)

    def third(r):
        def one(j, carry):
            own_ref[r, j, : held_rows(r)] = product(r, 12 + j)
            return carry

        lax.fori_loop(0, 4, one, 0)

    def add_first(r):
        got(r, 4, 4, near_sem.at[r])
        for j in range(4):
            count = held_rows(r)
            own_ref[r, j, :count] = own_ref[r, j, :count] + got_ref[r, 4 + j, :count].astype(
                jnp.float32
            )

    def last(r):
        for j in range(4):
            got(r, 8 + j, 1, two_sem.at[r, j])
            at = path_sub(j)[1] * width
            total = (
                own_ref[r, j, : held_rows(r)]
                + got_ref[r, 8 + j, : held_rows(r)].astype(jnp.float32)
            ).astype(out_ref.dtype)
            if r:
                out_ref[span:, at : at + width] = total
            else:
                out_ref[:kept, at : at + width] = total[:kept]

                @pl.when(middle)
                def _():
                    out_ref[kept:span, at : at + width] = total[kept:span]
                    back_out[:, at : at + width] = total[span:]

    def normalise(r, h):
        for head in range(h * shared, (h + 1) * shared):
            att_ref[r, :span, head * HEAD_DIM : (head + 1) * HEAD_DIM] = part.result(
                head, r * span, span
            )
        if r == 0:
            lent = part.finished(part.more_acc[h])
            for u in range(shared):
                at = (h * shared + u) * HEAD_DIM
                att_ref[0, span:, at : at + HEAD_DIM] = lent[u * extra : (u + 1) * extra]

    with jax.named_scope("begin"):
        part.start()
    for i in range(pieces):
        fetch(i, block_of(i), path_sub(i)[1]).start()
    with jax.named_scope("prepare"):
        part.prepare()
    part.slots(0, 3, False)
    with jax.named_scope("lent"):
        pl.when(middle)(part.catch_up)
    part.slots(3, 4, True)
    part.slots(4, 6, True, span)
    fetched(0)
    chip = part.chip_of(3)
    part.look(chip)
    block, own, partners = (
        chip * CORES, chip * CORES + part.core, chip * CORES + 1 - part.core
    )

    def whole(h):
        part.arrived(h, chip, 1 - part.core)
        part.turn(block, CORES, h)
        part.attend(block, CORES, h, 0, span, lent=True)

    def halves(h):
        if h:
            with jax.named_scope("pass_on"):
                part.pass_on(3, h)
        with jax.named_scope("own_half"):
            part.turn(own, 1, h)
            part.attend(own, 1, h, 0, span)
        if h == kv_heads - 1:
            with jax.named_scope("early"):
                early_products()
        with jax.named_scope("arrive"):
            part.arrived(h, chip, 1 - part.core)
        with jax.named_scope("other_half"):
            part.turn(partners, 1, h)
            part.attend(partners, 1, h, 0, span)

    for h in range(kv_heads):
        with jax.named_scope("attend_0"):
            pl.when(middle)(functools.partial(whole, h))
            pl.when(jnp.logical_not(middle))(functools.partial(halves, h))
        with jax.named_scope("norm"):
            normalise(0, h)
    with jax.named_scope("first_0"):
        pl.when(middle)(lambda: first_far(0, 0, 2))
        pl.when(jnp.logical_not(middle))(late_products)
        first_far(0, 2, 4)
        first_near(0)
    with jax.named_scope("attend_1"):
        for h in range(kv_heads):
            part.attend(block, CORES, h, span, span)

        def put_off(k, carry):
            before, held = part.plan(k)[4:]
            part.look(before)
            part.turn(before * CORES, CORES, held)
            part.attend(before * CORES, CORES, held, span, span)
            return carry

        lax.fori_loop(4, 6, put_off, 0)
        for h in range(kv_heads):
            normalise(1, h)
    with jax.named_scope("first_1_far"):
        first_far(1)
        fetched(1)
    with jax.named_scope("second_0"):
        second(0)
    with jax.named_scope("first_1_near"):
        first_near(1)
    with jax.named_scope("third_0"):
        third(0)
    with jax.named_scope("second_1"):
        second(1)
    with jax.named_scope("third_1"):
        third(1)
    with jax.named_scope("add_0"):
        add_first(0)
    with jax.named_scope("last_0"):
        last(0)
        pl.when(middle)(lambda: give_back().start())
    with jax.named_scope("add_1"):
        add_first(1)
    with jax.named_scope("last_1"):
        last(1)
    with jax.named_scope("drain"):
        @pl.when(middle)
        def _():
            give_back().wait_send()

        @pl.when(jnp.logical_not(middle))
        def _():
            give_back().wait_recv()
            out_ref[kept:span] = back_in[...]
            part.lend().wait_send()

        for r in range(spans):
            sent(r)
        part.drain()


def fused(queries, keys, values, out_weight, span_order, document, n_ctx, kv_heads, first_of):
    slots = span_order.shape[0]
    span = document.shape[0] // slots
    rows, depth = queries.shape
    features = out_weight.shape[1]
    width = features // 16
    spans = rows // span
    heads = depth // HEAD_DIM
    extra = HEAD_DIM * kv_heads // heads
    most = span + extra
    f32, bf16 = jnp.float32, jnp.bfloat16
    hbm = pl.BlockSpec(memory_space=pl.ANY)
    vmem = pl.BlockSpec(memory_space=pltpu.VMEM)
    return pl.pallas_call(
        functools.partial(fused_kernel, n_ctx, kv_heads, first_of),
        out_shape=pltpu.VMEM((rows, features // 4), bf16),
        in_specs=[hbm] * 6,
        out_specs=vmem,
        scratch_shapes=[
            pltpu.VMEM((spans, most, depth), bf16),
            pltpu.VMEM((16, depth, width), bf16),
            pltpu.VMEM((spans, 12, most, width), bf16),
            pltpu.VMEM((spans, 12, most, width), bf16),
            pltpu.VMEM((spans, 4, most, width), f32),
            pltpu.VMEM((extra, features // 4), bf16),
            pltpu.VMEM((extra, features // 4), bf16),
            pltpu.SemaphoreType.DMA((2,)),
            pltpu.SemaphoreType.DMA((spans,)),
            pltpu.SemaphoreType.DMA((spans, 4)),
            pltpu.SemaphoreType.DMA((spans,)),
            pltpu.SemaphoreType.DMA((spans, 4)),
            pltpu.SemaphoreType.DMA((2,)),
        ]
        + attention_scratch(n_ctx, slots, rows, heads, kv_heads, span)
        + [
            pltpu.VMEM((extra, depth), bf16),
            pltpu.VMEM((kv_heads, HEAD_DIM, HEAD_DIM), bf16),
            pltpu.VMEM((8, span), jnp.int32),
            pltpu.VMEM((CORES * rows, HEAD_DIM), f32),
            pltpu.VMEM((kv_heads, 1, HEAD_DIM), f32),
            pltpu.VMEM((kv_heads, HEAD_DIM + ONES, HEAD_DIM), f32),
            pltpu.SemaphoreType.DMA((3,)),
        ],
        compiler_params=pltpu.CompilerParams(
            collective_id=0, has_side_effects=True, vmem_limit_bytes=60 * 1024 * 1024
        ),
        name="attend_project",
    )(span_order, document.reshape(slots, 1, span), queries, keys, values, out_weight)


def gather_attend(queries, keys, values, span_order, document, n_ctx, kv_heads, first_of):
    slots = span_order.shape[0]
    span = document.shape[0] // slots
    rows, depth = queries.shape
    hbm = pl.BlockSpec(memory_space=pl.ANY)
    vmem = pl.BlockSpec(memory_space=pltpu.VMEM)
    return pl.pallas_call(
        functools.partial(gather_attend_kernel, n_ctx, kv_heads, first_of),
        out_shape=jax.ShapeDtypeStruct(queries.shape, queries.dtype),
        in_specs=[hbm] * 5,
        out_specs=vmem,
        scratch_shapes=attention_scratch(n_ctx, slots, rows, depth // HEAD_DIM, kv_heads, span),
        compiler_params=pltpu.CompilerParams(collective_id=0, has_side_effects=True),
        name="gather_attend",
    )(span_order, document.reshape(slots, 1, span), queries, keys, values)


def shards(n_ctx, n_grp, queries, keys, values, out_weight, span_order, document):
    local_heads = queries.shape[1] // HEAD_DIM
    kv_heads = max(1, local_heads // QUERY_GROUP)

    def first_of(group):
        return group * local_heads // QUERY_GROUP

    spans = queries.shape[0] * span_order.shape[0] // document.shape[0]
    if n_grp == 4 and n_ctx == 4 * CORES and kv_heads == 2 and spans == 2:
        return fused(
            queries, keys, values, out_weight, span_order, document, n_ctx, kv_heads, first_of
        )
    attended = gather_attend(
        queries, keys, values, span_order, document, n_ctx, kv_heads, first_of
    )
    partial_value = jnp.dot(attended, out_weight, preferred_element_type=jnp.float32)
    return lax.psum_scatter(
        partial_value.astype(jnp.bfloat16), "grp", scatter_dimension=1, tiled=True
    )


def solution(mesh):
    in_specs = (P("ctx", "grp"), P("ctx", None), P("ctx", None), P("grp", None), P(), P())
    body = functools.partial(shards, mesh.shape["ctx"], mesh.shape["grp"])
    return jax.shard_map(
        body, mesh=mesh, in_specs=in_specs, out_specs=P("ctx", "grp"), check_vma=False
    )
```
